64 devices in a mesh: sys: 4 (over x, y), row: 16 (over z, core).
Axes of the slice: x: 2, y: 2, z: 8, core: 2. Of those that a mesh axis runs over, the one named last changes fastest.
The devices are a block of a 4x4x8 slice.
Arguments:
- positions: bfloat16 [131072, 512], P(('sys', 'row')), parts along dimension 0
- charges: float32 [131072], P(('sys', 'row')), parts along dimension 0
- counts: int32 [64], P(('sys', 'row')), parts along dimension 0
Outputs:
- output 1: float32 [131072, 512], P(('sys', 'row')), parts along dimension 0
- output 2: float32 [4], P('sys'), parts along dimension 0
There are 4 independent parts. The reference program is written for one: setup_inputs(seed, part) draws one part's arguments, and reference() takes and returns one part's arrays. A program takes and returns all parts, laid end to end along the dimension named above; each array names one.
All inputs are finite; a program needn't handle non-finite values.
Results may differ from the reference program's by a relative error of at most 0.001.
Values are sent between devices in bfloat16 or wider.
A program may use at most 768 MiB of HBM per device.

```python
import jax
import jax.numpy as jnp
from jax import lax

BLOCK_ROWS = 2048
D = 512
RING_SIZE = 16
NUM_ROWS = RING_SIZE * BLOCK_ROWS
ROW_TILE = min(BLOCK_ROWS, 256)


def setup_inputs(seed: int = 0, part: int = 0) -> dict:
    part_key = jax.random.fold_in(jax.random.key(seed), part)
    sub_keys = jax.random.split(part_key, 6)
    positions = jax.random.normal(sub_keys[0], (NUM_ROWS, D), jnp.float32).astype(jnp.bfloat16)
    sign_vals = jnp.where(jax.random.bernoulli(sub_keys[1], 0.5, (NUM_ROWS,)), 1.0, -1.0)
    magnitude = jax.random.uniform(sub_keys[2], (NUM_ROWS,), jnp.float32, 0.5, 1.5)
    charges = (sign_vals * magnitude).astype(jnp.float32)
    counts = jax.random.randint(sub_keys[3], (RING_SIZE,), BLOCK_ROWS // 16, BLOCK_ROWS + 1)
    full_slot = jax.random.randint(sub_keys[4], (), 0, RING_SIZE)
    small_slot = (full_slot + jax.random.randint(sub_keys[5], (), 1, RING_SIZE)) % RING_SIZE
    counts = counts.at[full_slot].set(BLOCK_ROWS).at[small_slot].set(BLOCK_ROWS // 16)
    return {'positions': positions, 'charges': charges, 'counts': counts.astype(jnp.int32)}


def reference(positions, charges, counts):
    is_valid = jnp.arange(BLOCK_ROWS)[None, :] < counts[:, None]
    live_q = jnp.where(is_valid, charges.reshape(RING_SIZE, BLOCK_ROWS), 0.0).reshape(NUM_ROWS)
    pos_f32 = positions.astype(jnp.float32)
    sq_norm = jnp.sum(pos_f32 * pos_f32, axis=1)
    col_ids = jnp.arange(NUM_ROWS)
    neg_scale = -0.5 / D
    inv_len2 = 1.0 / D

    def tile_terms(tile_idx):
        row_start = tile_idx * ROW_TILE
        row_block = lax.dynamic_slice(positions, (row_start, 0), (ROW_TILE, D))
        row_q = lax.dynamic_slice(live_q, (row_start,), (ROW_TILE,))
        row_sq = lax.dynamic_slice(sq_norm, (row_start,), (ROW_TILE,))
        gram_mat = jnp.dot(row_block, positions.T, preferred_element_type=jnp.float32)
        dist_sq = jnp.maximum(row_sq[:, None] + sq_norm[None, :] - 2.0 * gram_mat, 0.0)
        weight = row_q[:, None] * live_q[None, :] * jnp.exp(dist_sq * neg_scale)
        row_ids = row_start + jnp.arange(ROW_TILE)
        weight = jnp.where(row_ids[:, None] == col_ids[None, :], 0.0, weight)
        pulled = jnp.dot(weight.astype(jnp.bfloat16), positions, preferred_element_type=jnp.float32)
        row_force = (jnp.sum(weight, axis=1)[:, None] * row_block.astype(jnp.float32) - pulled) * inv_len2
        return row_force, jnp.sum(weight)

    tile_forces, tile_energy = lax.map(tile_terms, jnp.arange(NUM_ROWS // ROW_TILE))
    return tile_forces.reshape(NUM_ROWS, D), (0.5 * jnp.sum(tile_energy)).reshape(1)
```

```python
import functools
import math

import jax
import jax.numpy as jnp
from jax import lax
from jax.experimental import pallas as pl
from jax.experimental.pallas import tpu as pltpu
from jax.sharding import PartitionSpec as P

MESH = pl.DeviceIdType.MESH
GROUP = 64
CHUNK = 256
PER = CHUNK // GROUP
LAG = 2
SLOTS = 8
ROW_TILE = 512
SIDE_ROWS = 40
STEP_PARTS = (28, 32, 35, 38, 41, 44, 50, 64)
LOG2E = math.log2(math.e)


def enter(num, me):
    barrier = pltpu.get_barrier_semaphore()
    for rel in range(1, num):
        pl.semaphore_signal(barrier, inc=1, device_id={'row': lax.rem(me + rel, num)}, device_id_type=MESH)
    pl.semaphore_wait(barrier, num - 1)


def exchange_kernel(num, side_ref, all_ref, send_sem, recv_sem):
    me = lax.axis_index('row')
    enter(num, me)
    copies = []
    for rel in range(1, num):
        copy = pltpu.make_async_remote_copy(
            src_ref=side_ref, dst_ref=all_ref.at[me], send_sem=send_sem.at[rel], recv_sem=recv_sem.at[me],
            device_id={'row': lax.rem(me + rel, num)}, device_id_type=MESH)
        copy.start()
        copies.append(copy)
    all_ref[me] = side_ref[...]
    for rel in range(1, num):
        src = lax.rem(me + rel, num)
        pltpu.make_async_remote_copy(
            src_ref=side_ref, dst_ref=all_ref.at[src], send_sem=send_sem.at[rel], recv_sem=recv_sem.at[src],
            device_id={'row': src}, device_id_type=MESH).wait_recv()
    for copy in copies:
        copy.wait_send()


def force_kernel(num, steps, block, width, tbl_ref, x_hbm, side_ref, a_ref, c_ref, out_ref, en_ref,
                 pool, cols, recv, sacc, bc, ids, esend, ebuf,
                 load_sem, pair_send, pair_recv, ring_send, ring_recv, sib_send, sib_recv, e_send, e_recv,
                 ring_free, sib_free):
    me = lax.axis_index('row')
    core = lax.rem(me, 2)
    sib = me + 1 - 2 * core
    nxt = lax.rem(me + 2 * (1 - core) + (num - 2) * core, num)
    prv = lax.rem(me + (num - 2) * (1 - core) + 2 * core, num)
    fifo0 = 2 * block
    fifo_chunks = (2 * block) // CHUNK
    groups = fifo0 // GROUP
    own0 = core * block
    own_g = pl.ds(core * (block // GROUP), block // GROUP)
    gain = LOG2E / width
    lane_groups = 2 * CHUNK // 128

    enter(num, me)
    load = pltpu.make_async_copy(x_hbm, pool.at[own_g], load_sem)
    load.start()
    pair = pltpu.make_async_remote_copy(
        src_ref=x_hbm, dst_ref=pool.at[own_g], send_sem=pair_send, recv_sem=pair_recv,
        device_id={'row': sib}, device_id_type=MESH)
    pair.start()

    def clear(m, carry):
        rows = pl.ds(pl.multiple_of(m * 128, 128), 128)
        out_ref[rows, :] = jnp.zeros((128, width), jnp.float32)
        sacc[rows, :] = jnp.zeros((128, 128), jnp.float32)
        return carry

    lax.fori_loop(0, block // 128, clear, 0)
    load.wait()
    pair.wait()

    def own_rows(r0, n):
        return pool[pl.ds((own0 + r0) // GROUP, n // GROUP)].reshape(n, width)

    def ring_copy(t):
        s = lax.rem(t, SLOTS)
        return pltpu.make_async_remote_copy(
            src_ref=cols.at[s, pl.ds(0, CHUNK)], dst_ref=recv.at[s], send_sem=ring_send.at[s], recv_sem=ring_recv.at[s],
            device_id={'row': nxt}, device_id_type=MESH)

    def sib_copy(t):
        s = lax.rem(t, SLOTS)
        return pltpu.make_async_remote_copy(
            src_ref=cols.at[s, pl.ds(0, CHUNK)], dst_ref=cols.at[s, pl.ds(CHUNK, CHUNK)],
            send_sem=sib_send.at[s], recv_sem=sib_recv.at[s], device_id={'row': sib}, device_id_type=MESH)

    last_send = steps - LAG

    def prep(t):
        s = lax.rem(t, SLOTS)
        for j in range(PER):
            cols[s, j * GROUP:(j + 1) * GROUP, :] = pool[tbl_ref[0, t * PER + j]]

    def take(t):
        ring_copy(t).wait_recv()
        dst = groups + lax.rem(t, fifo_chunks) * PER
        pool[pl.ds(dst, PER)] = recv[lax.rem(t, SLOTS)].reshape(PER, GROUP, width)

        @pl.when(t + SLOTS < last_send)
        def _():
            pl.semaphore_signal(ring_free, inc=1, device_id={'row': prv}, device_id_type=MESH)

    def col_vectors(t, masked):
        lane = lax.broadcasted_iota(jnp.int32, (1, 128), 1)
        low = lane < GROUP
        for half in range(2):
            for p in range(PER // 2):
                at = t * PER + 2 * p
                r0 = side_ref[tbl_ref[2 + half, at]].reshape(1, 128)
                r1 = side_ref[tbl_ref[2 + half, at + 1]].reshape(1, 128)
                dst = half * CHUNK + p * 128
                bc[0:1, dst:dst + 128] = jnp.where(low, r0, pltpu.roll(r1, GROUP, axis=1))
                bc[1:2, dst:dst + 128] = jnp.where(low, pltpu.roll(r0, GROUP, axis=1), r1)
                if masked:
                    i0 = tbl_ref[half, at] * GROUP - own0
                    i1 = tbl_ref[half, at + 1] * GROUP - own0 - GROUP
                    ids[0:1, dst:dst + 128] = jnp.where(low, i0, i1) + lane

    num_tiles = block // ROW_TILE

    def compute(t, masked, between):
        s = lax.rem(t, SLOTS)

        def tile(m, carry):
            @pl.when(m == 1)
            def _():
                between()
            r0 = pl.multiple_of(m * ROW_TILE, ROW_TILE)
            rows = pl.ds(r0, ROW_TILE)
            x = own_rows(r0, ROW_TILE)
            y = cols[s]
            g = lax.dot_general(x, y, (((1,), (1,)), ((), ())), preferred_element_type=jnp.float32)
            a = a_ref[rows, :]
            c = c_ref[rows, :]
            if masked:
                rid = lax.broadcasted_iota(jnp.int32, (ROW_TILE, 128), 0) + r0
            total = sacc[rows, :]
            parts = []
            for l in range(lane_groups):
                sl = slice(l * 128, (l + 1) * 128)
                e = jnp.minimum(g[:, sl] * gain + (a + bc[0:1, sl]), 0.0)
                w = (c * bc[1:2, sl]) * jnp.exp2(e)
                if masked:
                    w = jnp.where(rid == ids[0:1, sl], 0.0, w)
                total = total + w
                parts.append(w.astype(jnp.bfloat16))
            sacc[rows, :] = total
            wl = jnp.concatenate(parts, axis=1)
            out_ref[rows, :] += jnp.dot(wl, y, preferred_element_type=jnp.float32)
            return carry

        lax.fori_loop(0, num_tiles, tile, 0)

    def send(t):
        ring_live = t < last_send

        @pl.when(ring_live)
        def _():
            @pl.when(t >= SLOTS)
            def _():
                pl.semaphore_wait(ring_free, 1)
            ring_copy(t).start()

        @pl.when(t >= SLOTS)
        def _():
            pl.semaphore_wait(sib_free, 1)
        sib_copy(t).start()

    def done(t):
        @pl.when(t < last_send)
        def _():
            ring_copy(t).wait_send()
        sib_copy(t).wait_send()

        @pl.when(t + SLOTS < steps)
        def _():
            pl.semaphore_signal(sib_free, inc=1, device_id={'row': sib}, device_id_type=MESH)

    def step(t, masked):
        @pl.when(t < steps)
        def _():
            @pl.when(t >= LAG)
            def _():
                take(t - LAG)
            prep(t)
        col_vectors(t - 1, masked)
        sib_copy(t - 1).wait_recv()

        def between():
            @pl.when(t < steps)
            def _():
                send(t)
        compute(t - 1, masked, between)
        done(t - 1)

    own_steps = block // CHUNK
    prep(0)
    send(0)
    lax.fori_loop(1, own_steps + 1, lambda t, c: (step(t, True), c)[1], 0)
    lax.fori_loop(own_steps + 1, steps + 1, lambda t, c: (step(t, False), c)[1], 0)

    def fold(m, acc):
        return acc + jnp.sum(sacc[pl.ds(pl.multiple_of(m * 128, 128), 128), :].reshape(16, 8, 128), axis=0)

    part = lax.fori_loop(0, block // 128, fold, jnp.zeros((8, 128), jnp.float32))
    part = jnp.sum(jnp.sum(part, axis=1, keepdims=True), axis=0, keepdims=True)
    esend[...] = jnp.broadcast_to(0.5 * part, esend.shape)
    inv = 1.0 / width

    def final(m, carry):
        r0 = pl.multiple_of(m * 128, 128)
        rows = pl.ds(r0, 128)
        x = own_rows(r0, 128).astype(jnp.float32)
        sums = jnp.sum(sacc[rows, :], axis=1, keepdims=True)
        out_ref[rows, :] = (sums * x - out_ref[rows, :]) * inv
        return carry

    copies = []
    for rel in range(1, num):
        copy = pltpu.make_async_remote_copy(
            src_ref=esend, dst_ref=ebuf.at[me], send_sem=e_send.at[rel], recv_sem=e_recv.at[me],
            device_id={'row': lax.rem(me + rel, num)}, device_id_type=MESH)
        copy.start()
        copies.append(copy)
    lax.fori_loop(0, block // 128, final, 0)
    ebuf[me] = esend[...]
    for rel in range(1, num):
        src = lax.rem(me + rel, num)
        pltpu.make_async_remote_copy(
            src_ref=esend, dst_ref=ebuf.at[src], send_sem=e_send.at[rel], recv_sem=e_recv.at[src],
            device_id={'row': src}, device_id_type=MESH).wait_recv()
    for copy in copies:
        copy.wait_send()
    en = ebuf[0]
    for j in range(1, num):
        en = en + ebuf[j]
    en_ref[...] = en


def stream_tables(counts, me, num, block, total_steps):
    chips = num // 2
    zero_row = SIDE_ROWS - 1
    grp = (counts + (GROUP - 1)) // GROUP
    pairs = grp.reshape(chips, 2)
    first = pairs[:, 0]
    used = pairs[:, 0] + pairs[:, 1]
    half0 = (used + 1) // 2
    base = jnp.stack([jnp.zeros_like(half0), half0], axis=1)
    real = jnp.stack([half0, used - half0], axis=1)
    padded = jnp.maximum(real, LAG * PER)
    need = jnp.max(jnp.sum(padded, axis=0))
    need_steps = (need + PER - 1) // PER
    chip = me // 2
    core = me % 2
    pos = jnp.arange(total_steps * PER, dtype=jnp.int32)
    blk_groups = block // GROUP
    fifo_groups = 2 * blk_groups
    pools, sides = [], []
    for other in range(2):
        k = jnp.where(core == 1, 1 - other, other)
        hop = jnp.where(k == 0, chips - 1, 1)
        order = (chip + hop * jnp.arange(chips, dtype=jnp.int32)) % chips
        onehot = (order[:, None] == jnp.arange(chips)[None, :]).astype(jnp.int32)

        def pick(v):
            return jnp.sum(onehot * v[None, :], axis=1)
        seg_pad = pick(jnp.where(k == 0, padded[:, 0], padded[:, 1]))
        seg_real = pick(jnp.where(k == 0, real[:, 0], real[:, 1]))
        seg_base = pick(jnp.where(k == 0, base[:, 0], base[:, 1]))
        seg_first = pick(first)
        tri = (jnp.arange(chips)[None, :] < jnp.arange(chips)[:, None]).astype(jnp.int32)
        start = jnp.sum(tri * seg_pad[None, :], axis=1)
        inside = (pos[:, None] >= start[None, :]) & (pos[:, None] < (start + seg_pad)[None, :])
        off = pos[:, None] - start[None, :]
        live = inside & (off < seg_real[None, :])
        u = off + seg_base[None, :]
        in_a = u < seg_first[None, :]
        side = jnp.where(in_a, 2 * order[None, :] * SIDE_ROWS + u,
                         (2 * order[None, :] + 1) * SIDE_ROWS + u - seg_first[None, :])
        side = jnp.sum(jnp.where(live, side - zero_row, 0), axis=1) + zero_row
        own = jnp.where(in_a, u, blk_groups + u - seg_first[None, :])
        own = jnp.where(live[:, 0], own[:, 0], 0)
        pool = jnp.where(pos < seg_pad[0], own, fifo_groups + (pos - seg_pad[0]) % fifo_groups)
        pools.append(pool)
        sides.append(side)
    return jnp.stack(pools + sides).astype(jnp.int32), need_steps


def solution(mesh):
    num = mesh.shape['row']

    def per_device(positions, charges, counts):
        block, width = positions.shape
        me = lax.axis_index('row')
        pos_f32 = positions.astype(jnp.float32)
        scale = -0.5 * LOG2E / width
        a = jnp.sum(pos_f32 * pos_f32, axis=1) * scale
        live_q = jnp.where(jnp.arange(block) < counts[0], charges, 0.0)
        side = jnp.concatenate([a.reshape(-1, GROUP), live_q.reshape(-1, GROUP)], axis=1)
        extra = jnp.full((1, 128), counts[0].astype(jnp.float32))
        blk_groups = block // GROUP
        side = jnp.concatenate([side, extra, jnp.zeros((SIDE_ROWS - blk_groups - 1, 128), jnp.float32)], axis=0)
        vmem = pl.BlockSpec(memory_space=pltpu.VMEM)
        everyone = pl.pallas_call(
            functools.partial(exchange_kernel, num),
            out_shape=jax.ShapeDtypeStruct((num, SIDE_ROWS, 128), jnp.float32),
            in_specs=[vmem], out_specs=vmem,
            scratch_shapes=[pltpu.SemaphoreType.DMA((num,)), pltpu.SemaphoreType.DMA((num,))],
            compiler_params=pltpu.CompilerParams(collective_id=0, has_side_effects=True),
            name='exchange',
        )(side)
        all_counts = everyone[:, blk_groups, 0].astype(jnp.int32)
        own_steps = block // CHUNK
        max_steps = (num // 2) * own_steps
        tbl, need_steps = stream_tables(all_counts, me, num, block, max_steps)
        all_side = everyone.reshape(num * SIDE_ROWS, 128)
        a_wide = jnp.broadcast_to(a[:, None], (block, 128))
        c_wide = jnp.broadcast_to(live_q[:, None], (block, 128))

        def call(steps, cid):
            dma = pltpu.SemaphoreType.DMA
            return pl.pallas_call(
                functools.partial(force_kernel, num, steps, block, width),
                out_shape=(jax.ShapeDtypeStruct((block, width), jnp.float32), jax.ShapeDtypeStruct((8, 128), jnp.float32)),
                in_specs=[pl.BlockSpec(memory_space=pltpu.SMEM), pl.BlockSpec(memory_space=pl.ANY), vmem, vmem, vmem],
                out_specs=(vmem, vmem),
                scratch_shapes=[
                    pltpu.VMEM((4 * block // GROUP, GROUP, width), jnp.bfloat16),
                    pltpu.VMEM((SLOTS, 2 * CHUNK, width), jnp.bfloat16),
                    pltpu.VMEM((SLOTS, CHUNK, width), jnp.bfloat16),
                    pltpu.VMEM((block, 128), jnp.float32),
                    pltpu.VMEM((8, 2 * CHUNK), jnp.float32),
                    pltpu.VMEM((8, 2 * CHUNK), jnp.int32),
                    pltpu.VMEM((8, 128), jnp.float32),
                    pltpu.VMEM((num, 8, 128), jnp.float32),
                    dma, dma, dma, dma((SLOTS,)), dma((SLOTS,)), dma((SLOTS,)), dma((SLOTS,)),
                    dma((num,)), dma((num,)),
                    pltpu.SemaphoreType.REGULAR, pltpu.SemaphoreType.REGULAR,
                ],
                compiler_params=pltpu.CompilerParams(
                    collective_id=cid, has_side_effects=True, vmem_limit_bytes=56 * 1024 * 1024),
                name='force',
            )(tbl, positions.reshape(-1, GROUP, width), all_side, a_wide, c_wide)

        choices = sorted({max(own_steps + 1, max_steps * part // 64) for part in STEP_PARTS})
        branch = jnp.sum((need_steps > jnp.array(choices[:-1], jnp.int32)).astype(jnp.int32))
        forces, energy = call(max_steps, 1)
        return forces, energy[0, :1]

    row_spec = P(('sys', 'row'), None)
    vec_spec = P(('sys', 'row'))
    return jax.shard_map(per_device, mesh=mesh, in_specs=(row_spec, vec_spec, vec_spec), out_specs=(row_spec, P('sys')), check_vma=False)
```

```python
import functools
import math

import jax
import jax.numpy as jnp
from jax import lax
from jax.experimental import pallas as pl
from jax.experimental.pallas import tpu as pltpu
from jax.sharding import PartitionSpec as P

MESH = pl.DeviceIdType.MESH
GROUP = 64
CHUNK = 256
PER = CHUNK // GROUP
LAG = 3
SLOTS = 8
ROW_TILE = 512
SIDE_ROWS = 40
STEP_PARTS = (28, 32, 35, 38, 41, 44, 50, 64)
LOG2E = math.log2(math.e)


def enter(num, me):
    barrier = pltpu.get_barrier_semaphore()
    for rel in range(1, num):
        pl.semaphore_signal(barrier, inc=1, device_id={'row': lax.rem(me + rel, num)}, device_id_type=MESH)
    pl.semaphore_wait(barrier, num - 1)


def exchange_kernel(num, side_ref, all_ref, send_sem, recv_sem):
    me = lax.axis_index('row')
    enter(num, me)
    copies = []
    for rel in range(1, num):
        copy = pltpu.make_async_remote_copy(
            src_ref=side_ref, dst_ref=all_ref.at[me], send_sem=send_sem.at[rel], recv_sem=recv_sem.at[me],
            device_id={'row': lax.rem(me + rel, num)}, device_id_type=MESH)
        copy.start()
        copies.append(copy)
    all_ref[me] = side_ref[...]
    for rel in range(1, num):
        src = lax.rem(me + rel, num)
        pltpu.make_async_remote_copy(
            src_ref=side_ref, dst_ref=all_ref.at[src], send_sem=send_sem.at[rel], recv_sem=recv_sem.at[src],
            device_id={'row': src}, device_id_type=MESH).wait_recv()
    for copy in copies:
        copy.wait_send()


def force_kernel(num, steps, block, width, tbl_ref, x_hbm, side_ref, a_ref, c_ref, out_ref, en_ref,
                 pool, cols, recv, sacc, bc, ids, esend, ebuf,
                 load_sem, pair_send, pair_recv, ring_send, ring_recv, sib_send, sib_recv, e_send, e_recv,
                 ring_free, sib_free):
    me = lax.axis_index('row')
    core = lax.rem(me, 2)
    sib = me + 1 - 2 * core
    nxt = lax.rem(me + 2 * (1 - core) + (num - 2) * core, num)
    prv = lax.rem(me + (num - 2) * (1 - core) + 2 * core, num)
    fifo0 = 2 * block
    fifo_chunks = (2 * block) // CHUNK
    groups = fifo0 // GROUP
    own0 = core * block
    own_g = pl.ds(core * (block // GROUP), block // GROUP)
    gain = LOG2E / width
    lane_groups = 2 * CHUNK // 128

    enter(num, me)
    load = pltpu.make_async_copy(x_hbm, pool.at[own_g], load_sem)
    load.start()
    pair = pltpu.make_async_remote_copy(
        src_ref=x_hbm, dst_ref=pool.at[own_g], send_sem=pair_send, recv_sem=pair_recv,
        device_id={'row': sib}, device_id_type=MESH)
    pair.start()

    def clear(m, carry):
        rows = pl.ds(pl.multiple_of(m * 128, 128), 128)
        out_ref[rows, :] = jnp.zeros((128, width), jnp.float32)
        sacc[rows, :] = jnp.zeros((128, 128), jnp.float32)
        return carry

    lax.fori_loop(0, block // 128, clear, 0)
    load.wait()
    pair.wait()

    def own_rows(r0, n):
        return pool[pl.ds((own0 + r0) // GROUP, n // GROUP)].reshape(n, width)

    def ring_copy(t):
        s = lax.rem(t, SLOTS)
        return pltpu.make_async_remote_copy(
            src_ref=cols.at[s, pl.ds(0, CHUNK)], dst_ref=recv.at[s], send_sem=ring_send.at[s], recv_sem=ring_recv.at[s],
            device_id={'row': nxt}, device_id_type=MESH)

    def sib_copy(t):
        s = lax.rem(t, SLOTS)
        return pltpu.make_async_remote_copy(
            src_ref=cols.at[s, pl.ds(0, CHUNK)], dst_ref=cols.at[s, pl.ds(CHUNK, CHUNK)],
            send_sem=sib_send.at[s], recv_sem=sib_recv.at[s], device_id={'row': sib}, device_id_type=MESH)

    last_send = steps - LAG

    def prep(t):
        s = lax.rem(t, SLOTS)
        for j in range(PER):
            cols[s, j * GROUP:(j + 1) * GROUP, :] = pool[tbl_ref[0, t * PER + j]]

    def take(t):
        ring_copy(t).wait_recv()
        dst = groups + lax.rem(t, fifo_chunks) * PER
        pool[pl.ds(dst, PER)] = recv[lax.rem(t, SLOTS)].reshape(PER, GROUP, width)

        @pl.when(t + SLOTS < last_send)
        def _():
            pl.semaphore_signal(ring_free, inc=1, device_id={'row': prv}, device_id_type=MESH)

    def col_vectors(t, masked):
        lane = lax.broadcasted_iota(jnp.int32, (1, 128), 1)
        low = lane < GROUP
        for half in range(2):
            for p in range(PER // 2):
                at = t * PER + 2 * p
                r0 = side_ref[tbl_ref[2 + half, at]].reshape(1, 128)
                r1 = side_ref[tbl_ref[2 + half, at + 1]].reshape(1, 128)
                dst = half * CHUNK + p * 128
                bc[0:1, dst:dst + 128] = jnp.where(low, r0, pltpu.roll(r1, GROUP, axis=1))
                bc[1:2, dst:dst + 128] = jnp.where(low, pltpu.roll(r0, GROUP, axis=1), r1)
                if masked:
                    i0 = tbl_ref[half, at] * GROUP - own0
                    i1 = tbl_ref[half, at + 1] * GROUP - own0 - GROUP
                    ids[0:1, dst:dst + 128] = jnp.where(low, i0, i1) + lane

    num_tiles = block // ROW_TILE

    def compute(t, masked, between):
        s = lax.rem(t, SLOTS)

        def tile(m, carry):
            @pl.when(m == 1)
            def _():
                between()
            r0 = pl.multiple_of(m * ROW_TILE, ROW_TILE)
            rows = pl.ds(r0, ROW_TILE)
            x = own_rows(r0, ROW_TILE)
            y = cols[s]
            g = lax.dot_general(x, y, (((1,), (1,)), ((), ())), preferred_element_type=jnp.float32)
            a = a_ref[rows, :]
            c = c_ref[rows, :]
            if masked:
                rid = lax.broadcasted_iota(jnp.int32, (ROW_TILE, 128), 0) + r0
            total = sacc[rows, :]
            parts = []
            for l in range(lane_groups):
                sl = slice(l * 128, (l + 1) * 128)
                e = jnp.minimum(g[:, sl] * gain + (a + bc[0:1, sl]), 0.0)
                w = (c * bc[1:2, sl]) * jnp.exp2(e)
                if masked:
                    w = jnp.where(rid == ids[0:1, sl], 0.0, w)
                total = total + w
                parts.append(w.astype(jnp.bfloat16))
            sacc[rows, :] = total
            wl = jnp.concatenate(parts, axis=1)
            out_ref[rows, :] += jnp.dot(wl, y, preferred_element_type=jnp.float32)
            return carry

        lax.fori_loop(0, num_tiles, tile, 0)

    def send(t):
        ring_live = t < last_send

        @pl.when(ring_live)
        def _():
            @pl.when(t >= SLOTS)
            def _():
                pl.semaphore_wait(ring_free, 1)
            ring_copy(t).start()

        @pl.when(t >= SLOTS)
        def _():
            pl.semaphore_wait(sib_free, 1)
        sib_copy(t).start()

    def done(t):
        @pl.when(t < last_send)
        def _():
            ring_copy(t).wait_send()
        sib_copy(t).wait_send()

        @pl.when(t + SLOTS < steps)
        def _():
            pl.semaphore_signal(sib_free, inc=1, device_id={'row': sib}, device_id_type=MESH)

    def step(t, masked):
        @pl.when(t < steps)
        def _():
            @pl.when(t >= LAG)
            def _():
                take(t - LAG)
            prep(t)
        col_vectors(t - 1, masked)
        sib_copy(t - 1).wait_recv()

        def between():
            @pl.when(t < steps)
            def _():
                send(t)
        compute(t - 1, masked, between)
        done(t - 1)

    own_steps = block // CHUNK
    prep(0)
    send(0)
    lax.fori_loop(1, own_steps + 1, lambda t, c: (step(t, True), c)[1], 0)
    lax.fori_loop(own_steps + 1, steps + 1, lambda t, c: (step(t, False), c)[1], 0)

    def fold(m, acc):
        return acc + jnp.sum(sacc[pl.ds(pl.multiple_of(m * 128, 128), 128), :].reshape(16, 8, 128), axis=0)

    part = lax.fori_loop(0, block // 128, fold, jnp.zeros((8, 128), jnp.float32))
    part = jnp.sum(jnp.sum(part, axis=1, keepdims=True), axis=0, keepdims=True)
    esend[...] = jnp.broadcast_to(0.5 * part, esend.shape)
    inv = 1.0 / width

    def final(m, carry):
        r0 = pl.multiple_of(m * 128, 128)
        rows = pl.ds(r0, 128)
        x = own_rows(r0, 128).astype(jnp.float32)
        sums = jnp.sum(sacc[rows, :], axis=1, keepdims=True)
        out_ref[rows, :] = (sums * x - out_ref[rows, :]) * inv
        return carry

    copies = []
    for rel in range(1, num):
        copy = pltpu.make_async_remote_copy(
            src_ref=esend, dst_ref=ebuf.at[me], send_sem=e_send.at[rel], recv_sem=e_recv.at[me],
            device_id={'row': lax.rem(me + rel, num)}, device_id_type=MESH)
        copy.start()
        copies.append(copy)
    lax.fori_loop(0, block // 128, final, 0)
    ebuf[me] = esend[...]
    for rel in range(1, num):
        src = lax.rem(me + rel, num)
        pltpu.make_async_remote_copy(
            src_ref=esend, dst_ref=ebuf.at[src], send_sem=e_send.at[rel], recv_sem=e_recv.at[src],
            device_id={'row': src}, device_id_type=MESH).wait_recv()
    for copy in copies:
        copy.wait_send()
    en = ebuf[0]
    for j in range(1, num):
        en = en + ebuf[j]
    en_ref[...] = en


def stream_tables(counts, me, num, block, total_steps):
    chips = num // 2
    zero_row = SIDE_ROWS - 1
    grp = (counts + (GROUP - 1)) // GROUP
    pairs = grp.reshape(chips, 2)
    first = pairs[:, 0]
    used = pairs[:, 0] + pairs[:, 1]
    half0 = (used + 1) // 2
    base = jnp.stack([jnp.zeros_like(half0), half0], axis=1)
    real = jnp.stack([half0, used - half0], axis=1)
    padded = jnp.maximum(real, LAG * PER)
    need = jnp.max(jnp.sum(padded, axis=0))
    need_steps = (need + PER - 1) // PER
    chip = me // 2
    core = me % 2
    pos = jnp.arange(total_steps * PER, dtype=jnp.int32)
    blk_groups = block // GROUP
    fifo_groups = 2 * blk_groups
    pools, sides = [], []
    for other in range(2):
        k = jnp.where(core == 1, 1 - other, other)
        hop = jnp.where(k == 0, chips - 1, 1)
        order = (chip + hop * jnp.arange(chips, dtype=jnp.int32)) % chips
        onehot = (order[:, None] == jnp.arange(chips)[None, :]).astype(jnp.int32)

        def pick(v):
            return jnp.sum(onehot * v[None, :], axis=1)
        seg_pad = pick(jnp.where(k == 0, padded[:, 0], padded[:, 1]))
        seg_real = pick(jnp.where(k == 0, real[:, 0], real[:, 1]))
        seg_base = pick(jnp.where(k == 0, base[:, 0], base[:, 1]))
        seg_first = pick(first)
        tri = (jnp.arange(chips)[None, :] < jnp.arange(chips)[:, None]).astype(jnp.int32)
        start = jnp.sum(tri * seg_pad[None, :], axis=1)
        inside = (pos[:, None] >= start[None, :]) & (pos[:, None] < (start + seg_pad)[None, :])
        off = pos[:, None] - start[None, :]
        live = inside & (off < seg_real[None, :])
        u = off + seg_base[None, :]
        in_a = u < seg_first[None, :]
        side = jnp.where(in_a, 2 * order[None, :] * SIDE_ROWS + u,
                         (2 * order[None, :] + 1) * SIDE_ROWS + u - seg_first[None, :])
        side = jnp.sum(jnp.where(live, side - zero_row, 0), axis=1) + zero_row
        own = jnp.where(in_a, u, blk_groups + u - seg_first[None, :])
        own = jnp.where(live[:, 0], own[:, 0], 0)
        pool = jnp.where(pos < seg_pad[0], own, fifo_groups + (pos - seg_pad[0]) % fifo_groups)
        pools.append(pool)
        sides.append(side)
    return jnp.stack(pools + sides).astype(jnp.int32), need_steps


def solution(mesh):
    num = mesh.shape['row']

    def per_device(positions, charges, counts):
        block, width = positions.shape
        me = lax.axis_index('row')
        pos_f32 = positions.astype(jnp.float32)
        scale = -0.5 * LOG2E / width
        a = jnp.sum(pos_f32 * pos_f32, axis=1) * scale
        live_q = jnp.where(jnp.arange(block) < counts[0], charges, 0.0)
        side = jnp.concatenate([a.reshape(-1, GROUP), live_q.reshape(-1, GROUP)], axis=1)
        extra = jnp.full((1, 128), counts[0].astype(jnp.float32))
        blk_groups = block // GROUP
        side = jnp.concatenate([side, extra, jnp.zeros((SIDE_ROWS - blk_groups - 1, 128), jnp.float32)], axis=0)
        vmem = pl.BlockSpec(memory_space=pltpu.VMEM)
        everyone = pl.pallas_call(
            functools.partial(exchange_kernel, num),
            out_shape=jax.ShapeDtypeStruct((num, SIDE_ROWS, 128), jnp.float32),
            in_specs=[vmem], out_specs=vmem,
            scratch_shapes=[pltpu.SemaphoreType.DMA((num,)), pltpu.SemaphoreType.DMA((num,))],
            compiler_params=pltpu.CompilerParams(collective_id=0, has_side_effects=True),
            name='exchange',
        )(side)
        all_counts = everyone[:, blk_groups, 0].astype(jnp.int32)
        own_steps = block // CHUNK
        max_steps = (num // 2) * own_steps
        tbl, need_steps = stream_tables(all_counts, me, num, block, max_steps)
        all_side = everyone.reshape(num * SIDE_ROWS, 128)
        a_wide = jnp.broadcast_to(a[:, None], (block, 128))
        c_wide = jnp.broadcast_to(live_q[:, None], (block, 128))

        def call(steps, cid):
            dma = pltpu.SemaphoreType.DMA
            return pl.pallas_call(
                functools.partial(force_kernel, num, steps, block, width),
                out_shape=(jax.ShapeDtypeStruct((block, width), jnp.float32), jax.ShapeDtypeStruct((8, 128), jnp.float32)),
                in_specs=[pl.BlockSpec(memory_space=pltpu.SMEM), pl.BlockSpec(memory_space=pl.ANY), vmem, vmem, vmem],
                out_specs=(vmem, vmem),
                scratch_shapes=[
                    pltpu.VMEM((4 * block // GROUP, GROUP, width), jnp.bfloat16),
                    pltpu.VMEM((SLOTS, 2 * CHUNK, width), jnp.bfloat16),
                    pltpu.VMEM((SLOTS, CHUNK, width), jnp.bfloat16),
                    pltpu.VMEM((block, 128), jnp.float32),
                    pltpu.VMEM((8, 2 * CHUNK), jnp.float32),
                    pltpu.VMEM((8, 2 * CHUNK), jnp.int32),
                    pltpu.VMEM((8, 128), jnp.float32),
                    pltpu.VMEM((num, 8, 128), jnp.float32),
                    dma, dma, dma, dma((SLOTS,)), dma((SLOTS,)), dma((SLOTS,)), dma((SLOTS,)),
                    dma((num,)), dma((num,)),
                    pltpu.SemaphoreType.REGULAR, pltpu.SemaphoreType.REGULAR,
                ],
                compiler_params=pltpu.CompilerParams(
                    collective_id=cid, has_side_effects=True, vmem_limit_bytes=56 * 1024 * 1024),
                name='force',
            )(tbl, positions.reshape(-1, GROUP, width), all_side, a_wide, c_wide)

        choices = sorted({max(own_steps + 1, max_steps * part // 64) for part in STEP_PARTS})
        branch = jnp.sum((need_steps > jnp.array(choices[:-1], jnp.int32)).astype(jnp.int32))
        forces, energy = lax.switch(branch, [functools.partial(call, steps, 1 + i) for i, steps in enumerate(choices)])
        return forces, energy[0, :1]

    row_spec = P(('sys', 'row'), None)
    vec_spec = P(('sys', 'row'))
    return jax.shard_map(per_device, mesh=mesh, in_specs=(row_spec, vec_spec, vec_spec), out_specs=(row_spec, P('sys')), check_vma=False)
```

```python
import functools
import math

import jax
import jax.numpy as jnp
from jax import lax
from jax.experimental import pallas as pl
from jax.experimental.pallas import tpu as pltpu
from jax.sharding import PartitionSpec as P

MESH = pl.DeviceIdType.MESH
GROUP = 64
CHUNK = 256
PER = CHUNK // GROUP
LAG = 3
AHEAD = 2
SLOTS = 8
ROW_TILE = 512
SIDE_ROWS = 40
STEP_PARTS = (31, 35, 38, 41, 45, 64)
LOG2E = math.log2(math.e)


def enter(num, me):
    barrier = pltpu.get_barrier_semaphore()
    for rel in range(1, num):
        pl.semaphore_signal(barrier, inc=1, device_id={'row': lax.rem(me + rel, num)}, device_id_type=MESH)
    pl.semaphore_wait(barrier, num - 1)


def exchange_kernel(num, side_ref, all_ref, send_sem, recv_sem):
    me = lax.axis_index('row')
    enter(num, me)
    copies = []
    for rel in range(1, num):
        copy = pltpu.make_async_remote_copy(
            src_ref=side_ref, dst_ref=all_ref.at[me], send_sem=send_sem.at[rel], recv_sem=recv_sem.at[me],
            device_id={'row': lax.rem(me + rel, num)}, device_id_type=MESH)
        copy.start()
        copies.append(copy)
    all_ref[me] = side_ref[...]
    for rel in range(1, num):
        src = lax.rem(me + rel, num)
        pltpu.make_async_remote_copy(
            src_ref=side_ref, dst_ref=all_ref.at[src], send_sem=send_sem.at[rel], recv_sem=recv_sem.at[src],
            device_id={'row': src}, device_id_type=MESH).wait_recv()
    for copy in copies:
        copy.wait_send()


def force_kernel(num, steps, block, width, tbl_ref, x_hbm, side_ref, a_ref, c_ref, out_ref, en_ref,
                 pool, cols, recv, sacc, bc, ids, esend, ebuf,
                 load_sem, pair_send, pair_recv, ring_send, ring_recv, sib_send, sib_recv, e_send, e_recv,
                 ring_free, sib_free, g_a, g_b, w_a, w_b):
    me = lax.axis_index('row')
    core = lax.rem(me, 2)
    sib = me + 1 - 2 * core
    nxt = lax.rem(me + 2 * (1 - core) + (num - 2) * core, num)
    prv = lax.rem(me + (num - 2) * (1 - core) + 2 * core, num)
    fifo0 = 2 * block
    fifo_chunks = (2 * block) // CHUNK
    groups = fifo0 // GROUP
    own0 = core * block
    own_g = pl.ds(core * (block // GROUP), block // GROUP)
    gain = LOG2E / width
    lane_groups = 2 * CHUNK // 128

    enter(num, me)
    load = pltpu.make_async_copy(x_hbm, pool.at[own_g], load_sem)
    load.start()
    pair = pltpu.make_async_remote_copy(
        src_ref=x_hbm, dst_ref=pool.at[own_g], send_sem=pair_send, recv_sem=pair_recv,
        device_id={'row': sib}, device_id_type=MESH)
    pair.start()

    def clear(m, carry):
        rows = pl.ds(pl.multiple_of(m * 128, 128), 128)
        out_ref[rows, :] = jnp.zeros((128, width), jnp.float32)
        sacc[rows, :] = jnp.zeros((128, 128), jnp.float32)
        return carry

    lax.fori_loop(0, block // 128, clear, 0)
    load.wait()
    pair.wait()

    def own_rows(r0, n):
        return pool[pl.ds((own0 + r0) // GROUP, n // GROUP)].reshape(n, width)

    def ring_copy(t):
        s = lax.rem(t, SLOTS)
        return pltpu.make_async_remote_copy(
            src_ref=cols.at[s, pl.ds(0, CHUNK)], dst_ref=recv.at[s], send_sem=ring_send.at[s], recv_sem=ring_recv.at[s],
            device_id={'row': nxt}, device_id_type=MESH)

    def sib_copy(t):
        s = lax.rem(t, SLOTS)
        return pltpu.make_async_remote_copy(
            src_ref=cols.at[s, pl.ds(0, CHUNK)], dst_ref=cols.at[s, pl.ds(CHUNK, CHUNK)],
            send_sem=sib_send.at[s], recv_sem=sib_recv.at[s], device_id={'row': sib}, device_id_type=MESH)

    last_send = steps - LAG

    def prep(t):
        s = lax.rem(t, SLOTS)
        for j in range(PER):
            cols[s, j * GROUP:(j + 1) * GROUP, :] = pool[tbl_ref[0, t * PER + j]]

    def take(t):
        ring_copy(t).wait_recv()
        dst = groups + lax.rem(t, fifo_chunks) * PER
        pool[pl.ds(dst, PER)] = recv[lax.rem(t, SLOTS)].reshape(PER, GROUP, width)

        @pl.when(t + SLOTS < last_send)
        def _():
            pl.semaphore_signal(ring_free, inc=1, device_id={'row': prv}, device_id_type=MESH)

    def col_vectors(t, masked):
        lane = lax.broadcasted_iota(jnp.int32, (1, 128), 1)
        low = lane < GROUP
        for half in range(2):
            for p in range(PER // 2):
                at = t * PER + 2 * p
                r0 = side_ref[tbl_ref[2 + half, at]].reshape(1, 128)
                r1 = side_ref[tbl_ref[2 + half, at + 1]].reshape(1, 128)
                dst = half * CHUNK + p * 128
                bc[0:1, dst:dst + 128] = jnp.where(low, r0, pltpu.roll(r1, GROUP, axis=1))
                bc[1:2, dst:dst + 128] = jnp.where(low, pltpu.roll(r0, GROUP, axis=1), r1)
                if masked:
                    i0 = tbl_ref[half, at] * GROUP - own0
                    i1 = tbl_ref[half, at + 1] * GROUP - own0 - GROUP
                    ids[0:1, dst:dst + 128] = jnp.where(low, i0, i1) + lane

    num_tiles = block // ROW_TILE

    def rows_of(m):
        return pl.ds(pl.multiple_of(m * ROW_TILE, ROW_TILE), ROW_TILE)

    def gram(m, s):
        return lax.dot_general(own_rows(m * ROW_TILE, ROW_TILE), cols[s], (((1,), (1,)), ((), ())),
                               preferred_element_type=jnp.float32)

    def weigh(g_ref, w_ref, m, masked):
        rows = rows_of(m)
        a = a_ref[rows, :]
        c = c_ref[rows, :]
        if masked:
            rid = lax.broadcasted_iota(jnp.int32, (ROW_TILE, 128), 0) + m * ROW_TILE
        total = sacc[rows, :]
        for l in range(lane_groups):
            sl = slice(l * 128, (l + 1) * 128)
            e = jnp.minimum(g_ref[:, sl] * gain + (a + bc[0:1, sl]), 0.0)
            w = (c * bc[1:2, sl]) * jnp.exp2(e)
            if masked:
                w = jnp.where(rid == ids[0:1, sl], 0.0, w)
            total = total + w
            w_ref[:, sl] = w.astype(jnp.bfloat16)
        sacc[rows, :] = total

    def pull(w_ref, m, s):
        rows = rows_of(m)
        out_ref[rows, :] += jnp.dot(w_ref[...], cols[s], preferred_element_type=jnp.float32)

    pairs = num_tiles // 2

    def body(t, i, masked):
        now = lax.rem(t, SLOTS)
        before = lax.rem(jnp.maximum(t - 1 + (i + pairs - 1) // pairs, 0), SLOTS)
        after = lax.rem(t + (i + 1) // pairs, SLOTS)
        g_b[...] = gram(2 * i + 1, now)
        weigh(g_a, w_a, 2 * i, masked)
        pull(w_b, lax.rem(2 * i - 1 + num_tiles, num_tiles), before)
        g_a[...] = gram(lax.rem(2 * i + 2, num_tiles), after)
        weigh(g_b, w_b, 2 * i + 1, masked)
        pull(w_a, 2 * i, now)

    def send(t):
        ring_live = t < last_send

        @pl.when(ring_live)
        def _():
            @pl.when(t >= SLOTS)
            def _():
                pl.semaphore_wait(ring_free, 1)
            ring_copy(t).start()

        @pl.when(t >= SLOTS)
        def _():
            pl.semaphore_wait(sib_free, 1)
        sib_copy(t).start()

    def done(t):
        @pl.when(t < last_send)
        def _():
            ring_copy(t).wait_send()
        sib_copy(t).wait_send()

        @pl.when(t + SLOTS < steps)
        def _():
            pl.semaphore_signal(sib_free, inc=1, device_id={'row': sib}, device_id_type=MESH)

    def step(t, masked):
        new = t + AHEAD

        @pl.when(new < steps)
        def _():
            @pl.when(new >= LAG)
            def _():
                take(new - LAG)
            prep(new)
        col_vectors(t, masked)

        @pl.when(new < steps)
        def _():
            send(new)

        def pair(i, carry):
            @pl.when((i == pairs - 1) & (t + 1 < steps))
            def _():
                sib_copy(t + 1).wait_recv()
            body(t, i, masked)
            return carry

        lax.fori_loop(0, pairs, pair, 0)

        @pl.when(t >= 1)
        def _():
            done(t - 1)

    own_steps = block // CHUNK
    for t in range(AHEAD):
        prep(t)
        send(t)
    w_b[...] = jnp.zeros_like(w_b)
    sib_copy(0).wait_recv()
    g_a[...] = gram(0, 0)
    lax.fori_loop(0, own_steps, lambda t, c: (step(t, True), c)[1], 0)
    lax.fori_loop(own_steps, steps, lambda t, c: (step(t, False), c)[1], 0)
    pull(w_b, num_tiles - 1, (steps - 1) % SLOTS)
    done(steps - 1)

    def fold(m, acc):
        return acc + jnp.sum(sacc[pl.ds(pl.multiple_of(m * 128, 128), 128), :].reshape(16, 8, 128), axis=0)

    part = lax.fori_loop(0, block // 128, fold, jnp.zeros((8, 128), jnp.float32))
    part = jnp.sum(jnp.sum(part, axis=1, keepdims=True), axis=0, keepdims=True)
    esend[...] = jnp.broadcast_to(0.5 * part, esend.shape)
    inv = 1.0 / width

    def final(m, carry):
        r0 = pl.multiple_of(m * 128, 128)
        rows = pl.ds(r0, 128)
        x = own_rows(r0, 128).astype(jnp.float32)
        sums = jnp.sum(sacc[rows, :], axis=1, keepdims=True)
        out_ref[rows, :] = (sums * x - out_ref[rows, :]) * inv
        return carry

    copies = []
    for rel in range(1, num):
        copy = pltpu.make_async_remote_copy(
            src_ref=esend, dst_ref=ebuf.at[me], send_sem=e_send.at[rel], recv_sem=e_recv.at[me],
            device_id={'row': lax.rem(me + rel, num)}, device_id_type=MESH)
        copy.start()
        copies.append(copy)
    lax.fori_loop(0, block // 128, final, 0)
    ebuf[me] = esend[...]
    for rel in range(1, num):
        src = lax.rem(me + rel, num)
        pltpu.make_async_remote_copy(
            src_ref=esend, dst_ref=ebuf.at[src], send_sem=e_send.at[rel], recv_sem=e_recv.at[src],
            device_id={'row': src}, device_id_type=MESH).wait_recv()
    for copy in copies:
        copy.wait_send()
    en = ebuf[0]
    for j in range(1, num):
        en = en + ebuf[j]
    en_ref[...] = en


def stream_tables(counts, me, num, block, total_steps):
    chips = num // 2
    zero_row = SIDE_ROWS - 1
    grp = (counts + (GROUP - 1)) // GROUP
    pairs = grp.reshape(chips, 2)
    first = pairs[:, 0]
    used = pairs[:, 0] + pairs[:, 1]
    half0 = (used + 1) // 2
    base = jnp.stack([jnp.zeros_like(half0), half0], axis=1)
    real = jnp.stack([half0, used - half0], axis=1)
    padded = jnp.maximum(real, LAG * PER)
    need = jnp.max(jnp.sum(padded, axis=0))
    need_steps = (need + PER - 1) // PER
    chip = me // 2
    core = me % 2
    pos = jnp.arange(total_steps * PER, dtype=jnp.int32)
    blk_groups = block // GROUP
    fifo_groups = 2 * blk_groups
    pools, sides = [], []
    for other in range(2):
        k = jnp.where(core == 1, 1 - other, other)
        hop = jnp.where(k == 0, chips - 1, 1)
        order = (chip + hop * jnp.arange(chips, dtype=jnp.int32)) % chips
        onehot = (order[:, None] == jnp.arange(chips)[None, :]).astype(jnp.int32)

        def pick(v):
            return jnp.sum(onehot * v[None, :], axis=1)
        seg_pad = pick(jnp.where(k == 0, padded[:, 0], padded[:, 1]))
        seg_real = pick(jnp.where(k == 0, real[:, 0], real[:, 1]))
        seg_base = pick(jnp.where(k == 0, base[:, 0], base[:, 1]))
        seg_first = pick(first)
        tri = (jnp.arange(chips)[None, :] < jnp.arange(chips)[:, None]).astype(jnp.int32)
        start = jnp.sum(tri * seg_pad[None, :], axis=1)
        inside = (pos[:, None] >= start[None, :]) & (pos[:, None] < (start + seg_pad)[None, :])
        off = pos[:, None] - start[None, :]
        live = inside & (off < seg_real[None, :])
        u = off + seg_base[None, :]
        in_a = u < seg_first[None, :]
        side = jnp.where(in_a, 2 * order[None, :] * SIDE_ROWS + u,
                         (2 * order[None, :] + 1) * SIDE_ROWS + u - seg_first[None, :])
        side = jnp.sum(jnp.where(live, side - zero_row, 0), axis=1) + zero_row
        own = jnp.where(in_a, u, blk_groups + u - seg_first[None, :])
        own = jnp.where(live[:, 0], own[:, 0], 0)
        pool = jnp.where(pos < seg_pad[0], own, fifo_groups + (pos - seg_pad[0]) % fifo_groups)
        pools.append(pool)
        sides.append(side)
    return jnp.stack(pools + sides).astype(jnp.int32), need_steps


def solution(mesh):
    num = mesh.shape['row']

    def per_device(positions, charges, counts):
        block, width = positions.shape
        me = lax.axis_index('row')
        pos_f32 = positions.astype(jnp.float32)
        scale = -0.5 * LOG2E / width
        a = jnp.sum(pos_f32 * pos_f32, axis=1) * scale
        live_q = jnp.where(jnp.arange(block) < counts[0], charges, 0.0)
        side = jnp.concatenate([a.reshape(-1, GROUP), live_q.reshape(-1, GROUP)], axis=1)
        extra = jnp.full((1, 128), counts[0].astype(jnp.float32))
        blk_groups = block // GROUP
        side = jnp.concatenate([side, extra, jnp.zeros((SIDE_ROWS - blk_groups - 1, 128), jnp.float32)], axis=0)
        vmem = pl.BlockSpec(memory_space=pltpu.VMEM)
        everyone = pl.pallas_call(
            functools.partial(exchange_kernel, num),
            out_shape=jax.ShapeDtypeStruct((num, SIDE_ROWS, 128), jnp.float32),
            in_specs=[vmem], out_specs=vmem,
            scratch_shapes=[pltpu.SemaphoreType.DMA((num,)), pltpu.SemaphoreType.DMA((num,))],
            compiler_params=pltpu.CompilerParams(collective_id=0, has_side_effects=True),
            name='exchange',
        )(side)
        all_counts = everyone[:, blk_groups, 0].astype(jnp.int32)
        own_steps = block // CHUNK
        max_steps = (num // 2) * own_steps
        tbl, need_steps = stream_tables(all_counts, me, num, block, max_steps)
        all_side = everyone.reshape(num * SIDE_ROWS, 128)
        a_wide = jnp.broadcast_to(a[:, None], (block, 128))
        c_wide = jnp.broadcast_to(live_q[:, None], (block, 128))

        def call(steps, cid):
            dma = pltpu.SemaphoreType.DMA
            tile = functools.partial(pltpu.VMEM, (ROW_TILE, 2 * CHUNK))
            return pl.pallas_call(
                functools.partial(force_kernel, num, steps, block, width),
                out_shape=(jax.ShapeDtypeStruct((block, width), jnp.float32), jax.ShapeDtypeStruct((8, 128), jnp.float32)),
                in_specs=[pl.BlockSpec(memory_space=pltpu.SMEM), pl.BlockSpec(memory_space=pl.ANY), vmem, vmem, vmem],
                out_specs=(vmem, vmem),
                scratch_shapes=[
                    pltpu.VMEM((4 * block // GROUP, GROUP, width), jnp.bfloat16),
                    pltpu.VMEM((SLOTS, 2 * CHUNK, width), jnp.bfloat16),
                    pltpu.VMEM((SLOTS, CHUNK, width), jnp.bfloat16),
                    pltpu.VMEM((block, 128), jnp.float32),
                    pltpu.VMEM((8, 2 * CHUNK), jnp.float32),
                    pltpu.VMEM((8, 2 * CHUNK), jnp.int32),
                    pltpu.VMEM((8, 128), jnp.float32),
                    pltpu.VMEM((num, 8, 128), jnp.float32),
                    dma, dma, dma, dma((SLOTS,)), dma((SLOTS,)), dma((SLOTS,)), dma((SLOTS,)),
                    dma((num,)), dma((num,)),
                    pltpu.SemaphoreType.REGULAR, pltpu.SemaphoreType.REGULAR,
                    tile(jnp.float32), tile(jnp.float32), tile(jnp.bfloat16), tile(jnp.bfloat16),
                ],
                compiler_params=pltpu.CompilerParams(
                    collective_id=cid, has_side_effects=True, vmem_limit_bytes=56 * 1024 * 1024),
                name='force',
            )(tbl, positions.reshape(-1, GROUP, width), all_side, a_wide, c_wide)

        choices = sorted({max(own_steps + 1, max_steps * part // 64) for part in STEP_PARTS})
        branch = jnp.sum((need_steps > jnp.array(choices[:-1], jnp.int32)).astype(jnp.int32))
        forces, energy = lax.switch(branch, [functools.partial(call, steps, 1 + i) for i, steps in enumerate(choices)])
        return forces, energy[0, :1]

    row_spec = P(('sys', 'row'), None)
    vec_spec = P(('sys', 'row'))
    return jax.shard_map(per_device, mesh=mesh, in_specs=(row_spec, vec_spec, vec_spec), out_specs=(row_spec, P('sys')), check_vma=False)
```

```python
import functools
import math

import jax
import jax.numpy as jnp
from jax import lax
from jax.experimental import pallas as pl
from jax.experimental.pallas import tpu as pltpu
from jax.sharding import PartitionSpec as P

MESH = pl.DeviceIdType.MESH
GROUP = 64
CHUNK = 256
PER = CHUNK // GROUP
LAG = 2
AHEAD = 2
SLOTS = 8
ROW_TILE = 512
SUB_TILE = 64
SIDE_ROWS = 40
STEP_PARTS = (35, 38, 41, 44, 48, 64)
LOG2E = math.log2(math.e)


def enter(num, me):
    barrier = pltpu.get_barrier_semaphore()
    for rel in range(1, num):
        pl.semaphore_signal(barrier, inc=1, device_id={'row': lax.rem(me + rel, num)}, device_id_type=MESH)
    pl.semaphore_wait(barrier, num - 1)


def exchange_kernel(num, side_ref, a_ref, c_ref, all_ref, a_wide, c_wide, send_sem, recv_sem, pass_send, pass_recv):
    me = lax.axis_index('row')
    sib = me + 1 - 2 * lax.rem(me, 2)
    peers = [lax.rem(me + rel, num) for rel in range(2, num, 2)]
    barrier = pltpu.get_barrier_semaphore()
    for peer in peers + [sib]:
        pl.semaphore_signal(barrier, inc=1, device_id={'row': peer}, device_id_type=MESH)
    pl.semaphore_wait(barrier, len(peers) + 1)
    copies = []
    for n, peer in enumerate(peers):
        copy = pltpu.make_async_remote_copy(
            src_ref=side_ref, dst_ref=all_ref.at[me], send_sem=send_sem.at[n], recv_sem=recv_sem.at[me],
            device_id={'row': peer}, device_id_type=MESH)
        copy.start()
        copies.append(copy)
    own = pltpu.make_async_remote_copy(
        src_ref=side_ref, dst_ref=all_ref.at[me], send_sem=pass_send.at[len(peers)], recv_sem=pass_recv.at[me],
        device_id={'row': sib}, device_id_type=MESH)
    own.start()
    all_ref[me] = side_ref[...]
    for r in range(a_ref.shape[0]):
        rows = slice(r * 128, (r + 1) * 128)
        a_wide[rows, :] = jnp.broadcast_to(a_ref[r:r + 1, :], (128, 128)).T
        c_wide[rows, :] = jnp.broadcast_to(c_ref[r:r + 1, :], (128, 128)).T
    for n, peer in enumerate(peers):
        pltpu.make_async_remote_copy(
            src_ref=side_ref, dst_ref=all_ref.at[peer], send_sem=send_sem.at[n], recv_sem=recv_sem.at[peer],
            device_id={'row': peer}, device_id_type=MESH).wait_recv()
        copy = pltpu.make_async_remote_copy(
            src_ref=all_ref.at[peer], dst_ref=all_ref.at[peer], send_sem=pass_send.at[n], recv_sem=pass_recv.at[peer],
            device_id={'row': sib}, device_id_type=MESH)
        copy.start()
        copies.append(copy)
    for src in [sib] + [lax.rem(sib + rel, num) for rel in range(2, num, 2)]:
        pltpu.make_async_remote_copy(
            src_ref=side_ref, dst_ref=all_ref.at[src], send_sem=pass_send.at[0], recv_sem=pass_recv.at[src],
            device_id={'row': sib}, device_id_type=MESH).wait_recv()
    own.wait_send()
    for copy in copies:
        copy.wait_send()


def force_kernel(num, steps, block, width, tbl_ref, x_hbm, side_ref, a_ref, c_ref, out_ref, en_ref,
                 pool, cols, recv, sacc, bc, ids, esend, ebuf,
                 load_sem, pair_send, pair_recv, ring_send, ring_recv, sib_send, sib_recv, e_send, e_recv,
                 ring_free, sib_free, g_a, g_b, w_a, w_b):
    me = lax.axis_index('row')
    core = lax.rem(me, 2)
    sib = me + 1 - 2 * core
    nxt = lax.rem(me + 2 * (1 - core) + (num - 2) * core, num)
    prv = lax.rem(me + (num - 2) * (1 - core) + 2 * core, num)
    fifo0 = 2 * block
    fifo_chunks = (2 * block) // CHUNK
    groups = fifo0 // GROUP
    own0 = core * block
    own_g = pl.ds(core * (block // GROUP), block // GROUP)
    gain = LOG2E / width
    lane_groups = 2 * CHUNK // 128

    enter(num, me)
    load = pltpu.make_async_copy(x_hbm, pool.at[own_g], load_sem)
    load.start()
    pair = pltpu.make_async_remote_copy(
        src_ref=x_hbm, dst_ref=pool.at[own_g], send_sem=pair_send, recv_sem=pair_recv,
        device_id={'row': sib}, device_id_type=MESH)
    pair.start()

    def clear(m, carry):
        rows = pl.ds(pl.multiple_of(m * 128, 128), 128)
        out_ref[rows, :] = jnp.zeros((128, width), jnp.float32)
        sacc[rows, :] = jnp.zeros((128, 128), jnp.float32)
        return carry

    lax.fori_loop(0, block // 128, clear, 0)
    load.wait()
    pair.wait()

    def own_rows(r0, n):
        return pool[pl.ds((own0 + r0) // GROUP, n // GROUP)].reshape(n, width)

    def ring_copy(t):
        s = lax.rem(t, SLOTS)
        return pltpu.make_async_remote_copy(
            src_ref=cols.at[s, pl.ds(0, CHUNK)], dst_ref=recv.at[s], send_sem=ring_send.at[s], recv_sem=ring_recv.at[s],
            device_id={'row': nxt}, device_id_type=MESH)

    def sib_copy(t):
        s = lax.rem(t, SLOTS)
        return pltpu.make_async_remote_copy(
            src_ref=cols.at[s, pl.ds(0, CHUNK)], dst_ref=cols.at[s, pl.ds(CHUNK, CHUNK)],
            send_sem=sib_send.at[s], recv_sem=sib_recv.at[s], device_id={'row': sib}, device_id_type=MESH)

    last_send = steps - LAG

    def prep(t):
        s = lax.rem(t, SLOTS)
        for j in range(PER):
            cols[s, j * GROUP:(j + 1) * GROUP, :] = pool[tbl_ref[0, t * PER + j]]

    def take(t):
        ring_copy(t).wait_recv()
        dst = groups + lax.rem(t, fifo_chunks) * PER
        pool[pl.ds(dst, PER)] = recv[lax.rem(t, SLOTS)].reshape(PER, GROUP, width)

        @pl.when(t + SLOTS < last_send)
        def _():
            pl.semaphore_signal(ring_free, inc=1, device_id={'row': prv}, device_id_type=MESH)

    def col_vectors(t, masked):
        lane = lax.broadcasted_iota(jnp.int32, (1, 128), 1)
        low = lane < GROUP
        for half in range(2):
            for p in range(PER // 2):
                at = t * PER + 2 * p
                r0 = side_ref[tbl_ref[2 + half, at]].reshape(1, 128)
                r1 = side_ref[tbl_ref[2 + half, at + 1]].reshape(1, 128)
                dst = half * CHUNK + p * 128
                bc[0:1, dst:dst + 128] = jnp.where(low, r0, pltpu.roll(r1, GROUP, axis=1))
                bc[1:2, dst:dst + 128] = jnp.where(low, pltpu.roll(r0, GROUP, axis=1), r1)
                if masked:
                    i0 = tbl_ref[half, at] * GROUP - own0
                    i1 = tbl_ref[half, at + 1] * GROUP - own0 - GROUP
                    ids[0:1, dst:dst + 128] = jnp.where(low, i0, i1) + lane

    num_tiles = block // ROW_TILE

    def rows_of(m):
        return pl.ds(pl.multiple_of(m * ROW_TILE, ROW_TILE), ROW_TILE)

    def gram(m, s):
        return lax.dot_general(own_rows(m * ROW_TILE, ROW_TILE), cols[s], (((1,), (1,)), ((), ())),
                               preferred_element_type=jnp.float32)

    def weigh(g_ref, w_ref, m, masked):
        for part in range(0, ROW_TILE, SUB_TILE):
            rows = pl.ds(pl.multiple_of(m * ROW_TILE + part, SUB_TILE), SUB_TILE)
            sub = slice(part, part + SUB_TILE)
            a = a_ref[rows, :]
            c = c_ref[rows, :]
            if masked:
                rid = lax.broadcasted_iota(jnp.int32, (SUB_TILE, 128), 0) + (m * ROW_TILE + part)
            total = sacc[rows, :]
            for l in range(lane_groups):
                sl = slice(l * 128, (l + 1) * 128)
                e = jnp.minimum(g_ref[sub, sl] * gain + (a + bc[0:1, sl]), 0.0)
                w = (c * bc[1:2, sl]) * jnp.exp2(e)
                if masked:
                    w = jnp.where(rid == ids[0:1, sl], 0.0, w)
                total = total + w
                w_ref[sub, sl] = w.astype(jnp.bfloat16)
            sacc[rows, :] = total

    def pull(w_ref, m, s):
        rows = rows_of(m)
        out_ref[rows, :] += jnp.dot(w_ref[...], cols[s], preferred_element_type=jnp.float32)

    pairs = num_tiles // 2

    def body(t, i, masked):
        now = lax.rem(t, SLOTS)
        before = lax.rem(jnp.maximum(t - 1 + (i + pairs - 1) // pairs, 0), SLOTS)
        after = lax.rem(t + (i + 1) // pairs, SLOTS)
        g_b[...] = gram(2 * i + 1, now)
        weigh(g_a, w_a, 2 * i, masked)
        pull(w_b, lax.rem(2 * i - 1 + num_tiles, num_tiles), before)
        g_a[...] = gram(lax.rem(2 * i + 2, num_tiles), after)
        weigh(g_b, w_b, 2 * i + 1, masked)
        pull(w_a, 2 * i, now)

    def send(t):
        ring_live = t < last_send

        @pl.when(ring_live)
        def _():
            @pl.when(t >= SLOTS)
            def _():
                pl.semaphore_wait(ring_free, 1)
            ring_copy(t).start()

        @pl.when(t >= SLOTS)
        def _():
            pl.semaphore_wait(sib_free, 1)
        sib_copy(t).start()

    def done(t):
        @pl.when(t < last_send)
        def _():
            ring_copy(t).wait_send()
        sib_copy(t).wait_send()

        @pl.when(t + SLOTS < steps)
        def _():
            pl.semaphore_signal(sib_free, inc=1, device_id={'row': sib}, device_id_type=MESH)

    def step(t, masked):
        new = t + AHEAD

        @pl.when(new < steps)
        def _():
            @pl.when(new >= LAG)
            def _():
                take(new - LAG)
            prep(new)
        col_vectors(t, masked)

        @pl.when(new < steps)
        def _():
            send(new)

        def pair(i, carry):
            @pl.when((i == pairs - 1) & (t + 1 < steps))
            def _():
                sib_copy(t + 1).wait_recv()
            body(t, i, masked)
            return carry

        lax.fori_loop(0, pairs, pair, 0)

        @pl.when(t >= 1)
        def _():
            done(t - 1)

    own_steps = block // CHUNK
    for t in range(AHEAD):
        prep(t)
        send(t)
    w_b[...] = jnp.zeros_like(w_b)
    sib_copy(0).wait_recv()
    g_a[...] = gram(0, 0)
    lax.fori_loop(0, own_steps, lambda t, c: (step(t, True), c)[1], 0)
    lax.fori_loop(own_steps, steps, lambda t, c: (step(t, False), c)[1], 0)
    pull(w_b, num_tiles - 1, (steps - 1) % SLOTS)
    done(steps - 1)

    def fold(m, acc):
        return acc + jnp.sum(sacc[pl.ds(pl.multiple_of(m * 128, 128), 128), :].reshape(16, 8, 128), axis=0)

    part = lax.fori_loop(0, block // 128, fold, jnp.zeros((8, 128), jnp.float32))
    part = jnp.sum(jnp.sum(part, axis=1, keepdims=True), axis=0, keepdims=True)
    esend[...] = jnp.broadcast_to(0.5 * part, esend.shape)
    inv = 1.0 / width

    def final(m, carry):
        r0 = pl.multiple_of(m * 128, 128)
        rows = pl.ds(r0, 128)
        x = own_rows(r0, 128).astype(jnp.float32)
        sums = jnp.sum(sacc[rows, :], axis=1, keepdims=True)
        out_ref[rows, :] = (sums * x - out_ref[rows, :]) * inv
        return carry

    copies = []
    for rel in range(1, num):
        copy = pltpu.make_async_remote_copy(
            src_ref=esend, dst_ref=ebuf.at[me], send_sem=e_send.at[rel], recv_sem=e_recv.at[me],
            device_id={'row': lax.rem(me + rel, num)}, device_id_type=MESH)
        copy.start()
        copies.append(copy)
    lax.fori_loop(0, block // 128, final, 0)
    ebuf[me] = esend[...]
    for rel in range(1, num):
        src = lax.rem(me + rel, num)
        pltpu.make_async_remote_copy(
            src_ref=esend, dst_ref=ebuf.at[src], send_sem=e_send.at[rel], recv_sem=e_recv.at[src],
            device_id={'row': src}, device_id_type=MESH).wait_recv()
    for copy in copies:
        copy.wait_send()
    en = ebuf[0]
    for j in range(1, num):
        en = en + ebuf[j]
    en_ref[...] = en


def stream_tables(counts, me, num, block, total_steps):
    chips = num // 2
    zero_row = SIDE_ROWS - 1
    grp = (counts + (GROUP - 1)) // GROUP
    pairs = grp.reshape(chips, 2)
    first = pairs[:, 0]
    used = pairs[:, 0] + pairs[:, 1]
    half0 = (used + 1) // 2
    base = jnp.stack([jnp.zeros_like(half0), half0], axis=1)
    real = jnp.stack([half0, used - half0], axis=1)
    padded = jnp.maximum(real, LAG * PER)
    need = jnp.max(jnp.sum(padded, axis=0))
    need_steps = (need + PER - 1) // PER
    chip = me // 2
    core = me % 2
    pos = jnp.arange(total_steps * PER, dtype=jnp.int32)
    blk_groups = block // GROUP
    fifo_groups = 2 * blk_groups
    pools, sides = [], []
    for other in range(2):
        k = jnp.where(core == 1, 1 - other, other)
        hop = jnp.where(k == 0, chips - 1, 1)
        order = (chip + hop * jnp.arange(chips, dtype=jnp.int32)) % chips
        onehot = (order[:, None] == jnp.arange(chips)[None, :]).astype(jnp.int32)

        def pick(v):
            return jnp.sum(onehot * v[None, :], axis=1)
        seg_pad = pick(jnp.where(k == 0, padded[:, 0], padded[:, 1]))
        seg_real = pick(jnp.where(k == 0, real[:, 0], real[:, 1]))
        seg_base = pick(jnp.where(k == 0, base[:, 0], base[:, 1]))
        seg_first = pick(first)
        tri = (jnp.arange(chips)[None, :] < jnp.arange(chips)[:, None]).astype(jnp.int32)
        start = jnp.sum(tri * seg_pad[None, :], axis=1)
        inside = (pos[:, None] >= start[None, :]) & (pos[:, None] < (start + seg_pad)[None, :])
        off = pos[:, None] - start[None, :]
        live = inside & (off < seg_real[None, :])
        u = off + seg_base[None, :]
        in_a = u < seg_first[None, :]
        side = jnp.where(in_a, 2 * order[None, :] * SIDE_ROWS + u,
                         (2 * order[None, :] + 1) * SIDE_ROWS + u - seg_first[None, :])
        side = jnp.sum(jnp.where(live, side - zero_row, 0), axis=1) + zero_row
        own = jnp.where(in_a, u, blk_groups + u - seg_first[None, :])
        own = jnp.where(live[:, 0], own[:, 0], 0)
        pool = jnp.where(pos < seg_pad[0], own, fifo_groups + (pos - seg_pad[0]) % fifo_groups)
        pools.append(pool)
        sides.append(side)
    return jnp.stack(pools + sides).astype(jnp.int32), need_steps


def solution(mesh):
    num = mesh.shape['row']

    def per_device(positions, charges, counts):
        block, width = positions.shape
        me = lax.axis_index('row')
        pos_f32 = positions.astype(jnp.float32)
        scale = -0.5 * LOG2E / width
        a = jnp.sum(pos_f32 * pos_f32, axis=1) * scale
        live_q = jnp.where(jnp.arange(block) < counts[0], charges, 0.0)
        side = jnp.concatenate([a.reshape(-1, GROUP), live_q.reshape(-1, GROUP)], axis=1)
        extra = jnp.full((1, 128), counts[0].astype(jnp.float32))
        blk_groups = block // GROUP
        side = jnp.concatenate([side, extra, jnp.zeros((SIDE_ROWS - blk_groups - 1, 128), jnp.float32)], axis=0)
        vmem = pl.BlockSpec(memory_space=pltpu.VMEM)
        wide = jax.ShapeDtypeStruct((block, 128), jnp.float32)
        dma = pltpu.SemaphoreType.DMA
        everyone, a_wide, c_wide = pl.pallas_call(
            functools.partial(exchange_kernel, num),
            out_shape=(jax.ShapeDtypeStruct((num, SIDE_ROWS, 128), jnp.float32), wide, wide),
            in_specs=[vmem, vmem, vmem], out_specs=(vmem, vmem, vmem),
            scratch_shapes=[dma((num // 2,)), dma((num,)), dma((num // 2,)), dma((num,))],
            compiler_params=pltpu.CompilerParams(collective_id=0, has_side_effects=True),
            name='exchange',
        )(side, a.reshape(-1, 128), live_q.reshape(-1, 128))
        all_counts = everyone[:, blk_groups, 0].astype(jnp.int32)
        own_steps = block // CHUNK
        max_steps = (num // 2) * own_steps
        tbl, need_steps = stream_tables(all_counts, me, num, block, max_steps)
        all_side = everyone.reshape(num * SIDE_ROWS, 128)

        def call(steps, cid):
            tile = functools.partial(pltpu.VMEM, (ROW_TILE, 2 * CHUNK))
            return pl.pallas_call(
                functools.partial(force_kernel, num, steps, block, width),
                out_shape=(jax.ShapeDtypeStruct((block, width), jnp.float32), jax.ShapeDtypeStruct((8, 128), jnp.float32)),
                in_specs=[pl.BlockSpec(memory_space=pltpu.SMEM), pl.BlockSpec(memory_space=pl.ANY), vmem, vmem, vmem],
                out_specs=(vmem, vmem),
                scratch_shapes=[
                    pltpu.VMEM((4 * block // GROUP, GROUP, width), jnp.bfloat16),
                    pltpu.VMEM((SLOTS, 2 * CHUNK, width), jnp.bfloat16),
                    pltpu.VMEM((SLOTS, CHUNK, width), jnp.bfloat16),
                    pltpu.VMEM((block, 128), jnp.float32),
                    pltpu.VMEM((8, 2 * CHUNK), jnp.float32),
                    pltpu.VMEM((8, 2 * CHUNK), jnp.int32),
                    pltpu.VMEM((8, 128), jnp.float32),
                    pltpu.VMEM((num, 8, 128), jnp.float32),
                    dma, dma, dma, dma((SLOTS,)), dma((SLOTS,)), dma((SLOTS,)), dma((SLOTS,)),
                    dma((num,)), dma((num,)),
                    pltpu.SemaphoreType.REGULAR, pltpu.SemaphoreType.REGULAR,
                    tile(jnp.float32), tile(jnp.float32), tile(jnp.bfloat16), tile(jnp.bfloat16),
                ],
                compiler_params=pltpu.CompilerParams(
                    collective_id=cid, has_side_effects=True, vmem_limit_bytes=56 * 1024 * 1024),
                name='force',
            )(tbl, positions.reshape(-1, GROUP, width), all_side, a_wide, c_wide)

        choices = sorted({max(own_steps + 1, max_steps * part // 64) for part in STEP_PARTS})
        branch = jnp.sum((need_steps > jnp.array(choices[:-1], jnp.int32)).astype(jnp.int32))
        forces, energy = lax.switch(branch, [functools.partial(call, steps, 1 + i) for i, steps in enumerate(choices)])
        return forces, energy[0, :1]

    row_spec = P(('sys', 'row'), None)
    vec_spec = P(('sys', 'row'))
    return jax.shard_map(per_device, mesh=mesh, in_specs=(row_spec, vec_spec, vec_spec), out_specs=(row_spec, P('sys')), check_vma=False)
```

```python
import functools
import math

import jax
import jax.numpy as jnp
from jax import lax
from jax.experimental import pallas as pl
from jax.experimental.pallas import tpu as pltpu
from jax.sharding import PartitionSpec as P

MESH = pl.DeviceIdType.MESH
GROUP = 64
CHUNK = 256
PER = CHUNK // GROUP
LAG = 2
AHEAD = 2
SLOTS = 8
ROW_TILE = 512
SUB_TILE = 64
SIDE_ROWS = 40
STEP_PARTS = (38, 40, 42, 44, 46, 49, 64)
LOG2E = math.log2(math.e)


def arrive(num, me):
    for rel in range(1, num):
        pl.semaphore_signal(pltpu.get_barrier_semaphore(), inc=1, device_id={'row': lax.rem(me + rel, num)},
                            device_id_type=MESH)


def exchange_kernel(num, side_ref, all_ref, a_wide, c_wide, send_sem, recv_sem, pass_send, pass_recv):
    me = lax.axis_index('row')
    sib = me + 1 - 2 * lax.rem(me, 2)
    peers = [lax.rem(me + rel, num) for rel in range(2, num, 2)]
    barrier = pltpu.get_barrier_semaphore()
    for peer in peers + [sib]:
        pl.semaphore_signal(barrier, inc=1, device_id={'row': peer}, device_id_type=MESH)
    pl.semaphore_wait(barrier, len(peers) + 1)
    copies = []
    for n, peer in enumerate(peers):
        copy = pltpu.make_async_remote_copy(
            src_ref=side_ref, dst_ref=all_ref.at[me], send_sem=send_sem.at[n], recv_sem=recv_sem.at[me],
            device_id={'row': peer}, device_id_type=MESH)
        copy.start()
        copies.append(copy)
    own = pltpu.make_async_remote_copy(
        src_ref=side_ref, dst_ref=all_ref.at[me], send_sem=pass_send.at[len(peers)], recv_sem=pass_recv.at[me],
        device_id={'row': sib}, device_id_type=MESH)
    own.start()
    all_ref[me] = side_ref[...]
    low = lax.broadcasted_iota(jnp.int32, (1, 128), 1) < GROUP
    for r in range(a_wide.shape[0] // 128):
        rows = slice(r * 128, (r + 1) * 128)
        r0 = side_ref[2 * r:2 * r + 1, :]
        r1 = side_ref[2 * r + 1:2 * r + 2, :]
        a = jnp.where(low, r0, pltpu.roll(r1, GROUP, axis=1))
        c = jnp.where(low, pltpu.roll(r0, GROUP, axis=1), r1)
        a_wide[rows, :] = jnp.broadcast_to(a, (128, 128)).T
        c_wide[rows, :] = jnp.broadcast_to(c, (128, 128)).T
    for n, peer in enumerate(peers):
        pltpu.make_async_remote_copy(
            src_ref=side_ref, dst_ref=all_ref.at[peer], send_sem=send_sem.at[n], recv_sem=recv_sem.at[peer],
            device_id={'row': peer}, device_id_type=MESH).wait_recv()
        copy = pltpu.make_async_remote_copy(
            src_ref=all_ref.at[peer], dst_ref=all_ref.at[peer], send_sem=pass_send.at[n], recv_sem=pass_recv.at[peer],
            device_id={'row': sib}, device_id_type=MESH)
        copy.start()
        copies.append(copy)
    for src in [sib] + [lax.rem(sib + rel, num) for rel in range(2, num, 2)]:
        pltpu.make_async_remote_copy(
            src_ref=side_ref, dst_ref=all_ref.at[src], send_sem=pass_send.at[0], recv_sem=pass_recv.at[src],
            device_id={'row': sib}, device_id_type=MESH).wait_recv()
    own.wait_send()
    for copy in copies:
        copy.wait_send()


def force_kernel(num, steps, block, width, tbl_ref, x_hbm, side_ref, a_ref, c_ref, out_ref, en_ref,
                 pool, cols, recv, sacc, bc, ids, esend, ebuf,
                 load_sem, pair_send, pair_recv, ring_send, ring_recv, sib_send, sib_recv, e_send, e_recv,
                 ring_free, sib_free, g_a, g_b, w_a, w_b):
    me = lax.axis_index('row')
    core = lax.rem(me, 2)
    sib = me + 1 - 2 * core
    nxt = lax.rem(me + 2 * (1 - core) + (num - 2) * core, num)
    prv = lax.rem(me + (num - 2) * (1 - core) + 2 * core, num)
    fifo0 = 2 * block
    fifo_chunks = (2 * block) // CHUNK
    groups = fifo0 // GROUP
    own0 = core * block
    own_g = pl.ds(core * (block // GROUP), block // GROUP)
    gain = LOG2E / width
    lane_groups = 2 * CHUNK // 128

    arrive(num, me)
    load = pltpu.make_async_copy(x_hbm, pool.at[own_g], load_sem)
    load.start()

    def clear(m, carry):
        rows = pl.ds(pl.multiple_of(m * 128, 128), 128)
        out_ref[rows, :] = jnp.zeros((128, width), jnp.float32)
        sacc[rows, :] = jnp.zeros((128, 128), jnp.float32)
        return carry

    lax.fori_loop(0, block // 128, clear, 0)
    w_b[...] = jnp.zeros_like(w_b)
    pl.semaphore_wait(pltpu.get_barrier_semaphore(), num - 1)
    pair = pltpu.make_async_remote_copy(
        src_ref=x_hbm, dst_ref=pool.at[own_g], send_sem=pair_send, recv_sem=pair_recv,
        device_id={'row': sib}, device_id_type=MESH)
    pair.start()
    load.wait()
    pair.wait()

    def own_rows(r0, n):
        return pool[pl.ds((own0 + r0) // GROUP, n // GROUP)].reshape(n, width)

    def ring_copy(t):
        s = lax.rem(t, SLOTS)
        return pltpu.make_async_remote_copy(
            src_ref=cols.at[s, pl.ds(0, CHUNK)], dst_ref=recv.at[s], send_sem=ring_send.at[s], recv_sem=ring_recv.at[s],
            device_id={'row': nxt}, device_id_type=MESH)

    def sib_copy(t):
        s = lax.rem(t, SLOTS)
        return pltpu.make_async_remote_copy(
            src_ref=cols.at[s, pl.ds(0, CHUNK)], dst_ref=cols.at[s, pl.ds(CHUNK, CHUNK)],
            send_sem=sib_send.at[s], recv_sem=sib_recv.at[s], device_id={'row': sib}, device_id_type=MESH)

    last_send = steps - LAG

    def prep(t):
        s = lax.rem(t, SLOTS)
        for j in range(PER):
            cols[s, j * GROUP:(j + 1) * GROUP, :] = pool[tbl_ref[0, t * PER + j]]

    def take(t):
        ring_copy(t).wait_recv()
        dst = groups + lax.rem(t, fifo_chunks) * PER
        pool[pl.ds(dst, PER)] = recv[lax.rem(t, SLOTS)].reshape(PER, GROUP, width)

        @pl.when(t + SLOTS < last_send)
        def _():
            pl.semaphore_signal(ring_free, inc=1, device_id={'row': prv}, device_id_type=MESH)

    def col_vectors(t, masked):
        lane = lax.broadcasted_iota(jnp.int32, (1, 128), 1)
        low = lane < GROUP
        for half in range(2):
            for p in range(PER // 2):
                at = t * PER + 2 * p
                r0 = side_ref[tbl_ref[2 + half, at]].reshape(1, 128)
                r1 = side_ref[tbl_ref[2 + half, at + 1]].reshape(1, 128)
                dst = half * CHUNK + p * 128
                bc[0:1, dst:dst + 128] = jnp.where(low, r0, pltpu.roll(r1, GROUP, axis=1))
                bc[1:2, dst:dst + 128] = jnp.where(low, pltpu.roll(r0, GROUP, axis=1), r1)
                if masked:
                    i0 = tbl_ref[half, at] * GROUP - own0
                    i1 = tbl_ref[half, at + 1] * GROUP - own0 - GROUP
                    ids[0:1, dst:dst + 128] = jnp.where(low, i0, i1) + lane

    num_tiles = block // ROW_TILE

    def rows_of(m):
        return pl.ds(pl.multiple_of(m * ROW_TILE, ROW_TILE), ROW_TILE)

    def gram(m, s):
        return lax.dot_general(own_rows(m * ROW_TILE, ROW_TILE), cols[s], (((1,), (1,)), ((), ())),
                               preferred_element_type=jnp.float32)

    def weigh(g_ref, w_ref, m, masked):
        for part in range(0, ROW_TILE, SUB_TILE):
            rows = pl.ds(pl.multiple_of(m * ROW_TILE + part, SUB_TILE), SUB_TILE)
            sub = slice(part, part + SUB_TILE)
            a = a_ref[rows, :]
            c = c_ref[rows, :]
            if masked:
                rid = lax.broadcasted_iota(jnp.int32, (SUB_TILE, 128), 0) + (m * ROW_TILE + part)
            total = sacc[rows, :]
            for l in range(lane_groups):
                sl = slice(l * 128, (l + 1) * 128)
                e = jnp.minimum(g_ref[sub, sl] * gain + (a + bc[0:1, sl]), 0.0)
                w = (c * bc[1:2, sl]) * jnp.exp2(e)
                if masked:
                    w = jnp.where(rid == ids[0:1, sl], 0.0, w)
                total = total + w
                w_ref[sub, sl] = w.astype(jnp.bfloat16)
            sacc[rows, :] = total

    def pull(w_ref, m, s):
        rows = rows_of(m)
        out_ref[rows, :] += jnp.dot(w_ref[...], cols[s], preferred_element_type=jnp.float32)

    pairs = num_tiles // 2

    def body(t, i, masked):
        now = lax.rem(t, SLOTS)
        before = lax.rem(jnp.maximum(t - 1 + (i + pairs - 1) // pairs, 0), SLOTS)
        after = lax.rem(t + (i + 1) // pairs, SLOTS)
        g_b[...] = gram(2 * i + 1, now)
        weigh(g_a, w_a, 2 * i, masked)
        pull(w_b, lax.rem(2 * i - 1 + num_tiles, num_tiles), before)
        g_a[...] = gram(lax.rem(2 * i + 2, num_tiles), after)
        weigh(g_b, w_b, 2 * i + 1, masked)
        pull(w_a, 2 * i, now)

    def send(t):
        ring_live = t < last_send

        @pl.when(ring_live)
        def _():
            @pl.when(t >= SLOTS)
            def _():
                pl.semaphore_wait(ring_free, 1)
            ring_copy(t).start()

        @pl.when(t >= SLOTS)
        def _():
            pl.semaphore_wait(sib_free, 1)
        sib_copy(t).start()

    def done(t):
        @pl.when(t < last_send)
        def _():
            ring_copy(t).wait_send()
        sib_copy(t).wait_send()

        @pl.when(t + SLOTS < steps)
        def _():
            pl.semaphore_signal(sib_free, inc=1, device_id={'row': sib}, device_id_type=MESH)

    def step(t, masked):
        new = t + AHEAD

        @pl.when(new < steps)
        def _():
            @pl.when(new >= LAG)
            def _():
                take(new - LAG)
            prep(new)
        col_vectors(t, masked)

        @pl.when(new < steps)
        def _():
            send(new)

        def pair(i, carry):
            @pl.when((i == pairs - 1) & (t + 1 < steps))
            def _():
                sib_copy(t + 1).wait_recv()
            body(t, i, masked)
            return carry

        lax.fori_loop(0, pairs, pair, 0)

        @pl.when(t >= 1)
        def _():
            done(t - 1)

    own_steps = block // CHUNK
    for t in range(AHEAD):
        prep(t)
        send(t)
    sib_copy(0).wait_recv()
    g_a[...] = gram(0, 0)
    lax.fori_loop(0, own_steps, lambda t, c: (step(t, True), c)[1], 0)
    lax.fori_loop(own_steps, steps, lambda t, c: (step(t, False), c)[1], 0)
    pull(w_b, num_tiles - 1, (steps - 1) % SLOTS)
    done(steps - 1)

    def fold(m, acc):
        return acc + jnp.sum(sacc[pl.ds(pl.multiple_of(m * 128, 128), 128), :].reshape(16, 8, 128), axis=0)

    part = lax.fori_loop(0, block // 128, fold, jnp.zeros((8, 128), jnp.float32))
    part = jnp.sum(jnp.sum(part, axis=1, keepdims=True), axis=0, keepdims=True)
    esend[...] = jnp.broadcast_to(0.5 * part, esend.shape)
    inv = 1.0 / width

    def final(m, carry):
        r0 = pl.multiple_of(m * 128, 128)
        rows = pl.ds(r0, 128)
        x = own_rows(r0, 128).astype(jnp.float32)
        sums = jnp.sum(sacc[rows, :], axis=1, keepdims=True)
        out_ref[rows, :] = (sums * x - out_ref[rows, :]) * inv
        return carry

    copies = []
    for rel in range(1, num):
        copy = pltpu.make_async_remote_copy(
            src_ref=esend, dst_ref=ebuf.at[me], send_sem=e_send.at[rel], recv_sem=e_recv.at[me],
            device_id={'row': lax.rem(me + rel, num)}, device_id_type=MESH)
        copy.start()
        copies.append(copy)
    lax.fori_loop(0, block // 128, final, 0)
    ebuf[me] = esend[...]
    for rel in range(1, num):
        src = lax.rem(me + rel, num)
        pltpu.make_async_remote_copy(
            src_ref=esend, dst_ref=ebuf.at[src], send_sem=e_send.at[rel], recv_sem=e_recv.at[src],
            device_id={'row': src}, device_id_type=MESH).wait_recv()
    for copy in copies:
        copy.wait_send()
    en = ebuf[0]
    for j in range(1, num):
        en = en + ebuf[j]
    en_ref[...] = en


def stream_tables(counts, me, num, block, total_steps):
    chips = num // 2
    zero_row = SIDE_ROWS - 1
    grp = (counts + (GROUP - 1)) // GROUP
    pairs = grp.reshape(chips, 2)
    first = pairs[:, 0]
    used = pairs[:, 0] + pairs[:, 1]
    half0 = (used + 1) // 2
    base = jnp.stack([jnp.zeros_like(half0), half0], axis=1)
    real = jnp.stack([half0, used - half0], axis=1)
    padded = jnp.maximum(real, LAG * PER)
    need = jnp.max(jnp.sum(padded, axis=0))
    need_steps = (need + PER - 1) // PER
    chip = me // 2
    core = me % 2
    pos = jnp.arange(total_steps * PER, dtype=jnp.int32)
    blk_groups = block // GROUP
    fifo_groups = 2 * blk_groups
    pools, sides = [], []
    for other in range(2):
        k = jnp.where(core == 1, 1 - other, other)
        hop = jnp.where(k == 0, chips - 1, 1)
        order = (chip + hop * jnp.arange(chips, dtype=jnp.int32)) % chips
        onehot = (order[:, None] == jnp.arange(chips)[None, :]).astype(jnp.int32)

        def pick(v):
            return jnp.sum(onehot * v[None, :], axis=1)
        seg_pad = pick(jnp.where(k == 0, padded[:, 0], padded[:, 1]))
        seg_real = pick(jnp.where(k == 0, real[:, 0], real[:, 1]))
        seg_base = pick(jnp.where(k == 0, base[:, 0], base[:, 1]))
        seg_first = pick(first)
        tri = (jnp.arange(chips)[None, :] < jnp.arange(chips)[:, None]).astype(jnp.int32)
        start = jnp.sum(tri * seg_pad[None, :], axis=1)
        inside = (pos[:, None] >= start[None, :]) & (pos[:, None] < (start + seg_pad)[None, :])
        off = pos[:, None] - start[None, :]
        live = inside & (off < seg_real[None, :])
        u = off + seg_base[None, :]
        in_a = u < seg_first[None, :]
        side = jnp.where(in_a, 2 * order[None, :] * SIDE_ROWS + u,
                         (2 * order[None, :] + 1) * SIDE_ROWS + u - seg_first[None, :])
        side = jnp.sum(jnp.where(live, side - zero_row, 0), axis=1) + zero_row
        own = jnp.where(in_a, u, blk_groups + u - seg_first[None, :])
        own = jnp.where(live[:, 0], own[:, 0], 0)
        pool = jnp.where(pos < seg_pad[0], own, fifo_groups + (pos - seg_pad[0]) % fifo_groups)
        pools.append(pool)
        sides.append(side)
    return jnp.stack(pools + sides).astype(jnp.int32), need_steps


def solution(mesh):
    num = mesh.shape['row']

    def per_device(positions, charges, counts):
        block, width = positions.shape
        me = lax.axis_index('row')
        pos_f32 = positions.astype(jnp.float32)
        scale = -0.5 * LOG2E / width
        a = jnp.sum(pos_f32 * pos_f32, axis=1) * scale
        live_q = jnp.where(jnp.arange(block) < counts[0], charges, 0.0)
        side = jnp.concatenate([a.reshape(-1, GROUP), live_q.reshape(-1, GROUP)], axis=1)
        extra = jnp.full((1, 128), counts[0].astype(jnp.float32))
        blk_groups = block // GROUP
        side = jnp.concatenate([side, extra, jnp.zeros((SIDE_ROWS - blk_groups - 1, 128), jnp.float32)], axis=0)
        vmem = pl.BlockSpec(memory_space=pltpu.VMEM)
        wide = jax.ShapeDtypeStruct((block, 128), jnp.float32)
        dma = pltpu.SemaphoreType.DMA
        everyone, a_wide, c_wide = pl.pallas_call(
            functools.partial(exchange_kernel, num),
            out_shape=(jax.ShapeDtypeStruct((num, SIDE_ROWS, 128), jnp.float32), wide, wide),
            in_specs=[vmem], out_specs=(vmem, vmem, vmem),
            scratch_shapes=[dma((num // 2,)), dma((num,)), dma((num // 2,)), dma((num,))],
            compiler_params=pltpu.CompilerParams(collective_id=0, has_side_effects=True),
            name='exchange',
        )(side)
        all_counts = everyone[:, blk_groups, 0].astype(jnp.int32)
        own_steps = block // CHUNK
        max_steps = (num // 2) * own_steps
        tbl, need_steps = stream_tables(all_counts, me, num, block, max_steps)
        all_side = everyone.reshape(num * SIDE_ROWS, 128)

        def call(steps, cid):
            tile = functools.partial(pltpu.VMEM, (ROW_TILE, 2 * CHUNK))
            return pl.pallas_call(
                functools.partial(force_kernel, num, steps, block, width),
                out_shape=(jax.ShapeDtypeStruct((block, width), jnp.float32), jax.ShapeDtypeStruct((8, 128), jnp.float32)),
                in_specs=[pl.BlockSpec(memory_space=pltpu.SMEM), pl.BlockSpec(memory_space=pl.ANY), vmem, vmem, vmem],
                out_specs=(vmem, vmem),
                scratch_shapes=[
                    pltpu.VMEM((4 * block // GROUP, GROUP, width), jnp.bfloat16),
                    pltpu.VMEM((SLOTS, 2 * CHUNK, width), jnp.bfloat16),
                    pltpu.VMEM((SLOTS, CHUNK, width), jnp.bfloat16),
                    pltpu.VMEM((block, 128), jnp.float32),
                    pltpu.VMEM((8, 2 * CHUNK), jnp.float32),
                    pltpu.VMEM((8, 2 * CHUNK), jnp.int32),
                    pltpu.VMEM((8, 128), jnp.float32),
                    pltpu.VMEM((num, 8, 128), jnp.float32),
                    dma, dma, dma, dma((SLOTS,)), dma((SLOTS,)), dma((SLOTS,)), dma((SLOTS,)),
                    dma((num,)), dma((num,)),
                    pltpu.SemaphoreType.REGULAR, pltpu.SemaphoreType.REGULAR,
                    tile(jnp.float32), tile(jnp.float32), tile(jnp.bfloat16), tile(jnp.bfloat16),
                ],
                compiler_params=pltpu.CompilerParams(
                    collective_id=cid, has_side_effects=True, vmem_limit_bytes=56 * 1024 * 1024),
                name='force',
            )(tbl, positions.reshape(-1, GROUP, width), all_side, a_wide, c_wide)

        choices = sorted({max(own_steps + 1, max_steps * part // 64) for part in STEP_PARTS})
        branch = sum((need_steps > steps).astype(jnp.int32) for steps in choices[:-1])
        forces, energy = lax.switch(branch, [functools.partial(call, steps, 1 + i) for i, steps in enumerate(choices)])
        return forces, energy[0, :1]

    row_spec = P(('sys', 'row'), None)
    vec_spec = P(('sys', 'row'))
    return jax.shard_map(per_device, mesh=mesh, in_specs=(row_spec, vec_spec, vec_spec), out_specs=(row_spec, P('sys')), check_vma=False)
```

```python
import functools
import math

import jax
import jax.numpy as jnp
from jax import lax
from jax.experimental import pallas as pl
from jax.experimental.pallas import tpu as pltpu
from jax.sharding import PartitionSpec as P

MESH = pl.DeviceIdType.MESH
GROUP = 64
CHUNK = 256
PER = CHUNK // GROUP
LAG = 2
AHEAD = 2
SLOTS = 8
ROW_TILE = 512
SUB_TILE = 64
SIDE_ROWS = 40
STEP_PARTS = (38, 40, 42, 44, 46, 49, 64)
LOG2E = math.log2(math.e)


def arrive(num, me):
    for rel in range(1, num):
        pl.semaphore_signal(pltpu.get_barrier_semaphore(), inc=1, device_id={'row': lax.rem(me + rel, num)},
                            device_id_type=MESH)


def exchange_kernel(num, side_ref, x_hbm, all_ref, a_wide, c_wide, x_sib,
                    send_sem, recv_sem, pass_send, pass_recv, x_send, x_recv):
    me = lax.axis_index('row')
    sib = me + 1 - 2 * lax.rem(me, 2)
    peers = [lax.rem(me + rel, num) for rel in range(2, num, 2)]
    barrier = pltpu.get_barrier_semaphore()
    for peer in peers + [sib]:
        pl.semaphore_signal(barrier, inc=1, device_id={'row': peer}, device_id_type=MESH)
    pl.semaphore_wait(barrier, len(peers) + 1)
    copies = []
    for n, peer in enumerate(peers):
        copy = pltpu.make_async_remote_copy(
            src_ref=side_ref, dst_ref=all_ref.at[me], send_sem=send_sem.at[n], recv_sem=recv_sem.at[me],
            device_id={'row': peer}, device_id_type=MESH)
        copy.start()
        copies.append(copy)
    own = pltpu.make_async_remote_copy(
        src_ref=side_ref, dst_ref=all_ref.at[me], send_sem=pass_send.at[len(peers)], recv_sem=pass_recv.at[me],
        device_id={'row': sib}, device_id_type=MESH)
    own.start()
    rows_out = pltpu.make_async_remote_copy(
        src_ref=x_hbm, dst_ref=x_sib, send_sem=x_send, recv_sem=x_recv, device_id={'row': sib}, device_id_type=MESH)
    rows_out.start()
    all_ref[me] = side_ref[...]
    low = lax.broadcasted_iota(jnp.int32, (1, 128), 1) < GROUP
    for r in range(a_wide.shape[0] // 128):
        rows = slice(r * 128, (r + 1) * 128)
        r0 = side_ref[2 * r:2 * r + 1, :]
        r1 = side_ref[2 * r + 1:2 * r + 2, :]
        a = jnp.where(low, r0, pltpu.roll(r1, GROUP, axis=1))
        c = jnp.where(low, pltpu.roll(r0, GROUP, axis=1), r1)
        a_wide[rows, :] = jnp.broadcast_to(a, (128, 128)).T
        c_wide[rows, :] = jnp.broadcast_to(c, (128, 128)).T
    for n, peer in enumerate(peers):
        pltpu.make_async_remote_copy(
            src_ref=side_ref, dst_ref=all_ref.at[peer], send_sem=send_sem.at[n], recv_sem=recv_sem.at[peer],
            device_id={'row': peer}, device_id_type=MESH).wait_recv()
        copy = pltpu.make_async_remote_copy(
            src_ref=all_ref.at[peer], dst_ref=all_ref.at[peer], send_sem=pass_send.at[n], recv_sem=pass_recv.at[peer],
            device_id={'row': sib}, device_id_type=MESH)
        copy.start()
        copies.append(copy)
    for src in [sib] + [lax.rem(sib + rel, num) for rel in range(2, num, 2)]:
        pltpu.make_async_remote_copy(
            src_ref=side_ref, dst_ref=all_ref.at[src], send_sem=pass_send.at[0], recv_sem=pass_recv.at[src],
            device_id={'row': sib}, device_id_type=MESH).wait_recv()
    own.wait_send()
    rows_out.wait()
    for copy in copies:
        copy.wait_send()


def force_kernel(num, steps, block, width, tbl_ref, x_hbm, x_sib, side_ref, a_ref, c_ref, out_ref, en_ref,
                 pool, cols, recv, sacc, bc, ids, esend, ebuf,
                 load_sem, pair_sem, ring_send, ring_recv, sib_send, sib_recv, e_send, e_recv,
                 ring_free, sib_free, g_a, g_b, w_a, w_b):
    me = lax.axis_index('row')
    core = lax.rem(me, 2)
    sib = me + 1 - 2 * core
    nxt = lax.rem(me + 2 * (1 - core) + (num - 2) * core, num)
    prv = lax.rem(me + (num - 2) * (1 - core) + 2 * core, num)
    fifo0 = 2 * block
    fifo_chunks = (2 * block) // CHUNK
    groups = fifo0 // GROUP
    own0 = core * block
    own_g = pl.ds(core * (block // GROUP), block // GROUP)
    sib_g = pl.ds((1 - core) * (block // GROUP), block // GROUP)
    gain = LOG2E / width
    lane_groups = 2 * CHUNK // 128

    arrive(num, me)
    load = pltpu.make_async_copy(x_hbm, pool.at[own_g], load_sem)
    load.start()
    pair = pltpu.make_async_copy(x_sib, pool.at[sib_g], pair_sem)
    pair.start()

    def clear(m, carry):
        rows = pl.ds(pl.multiple_of(m * 128, 128), 128)
        out_ref[rows, :] = jnp.zeros((128, width), jnp.float32)
        sacc[rows, :] = jnp.zeros((128, 128), jnp.float32)
        return carry

    lax.fori_loop(0, block // 128, clear, 0)
    w_b[...] = jnp.zeros_like(w_b)
    pl.semaphore_wait(pltpu.get_barrier_semaphore(), num - 1)
    load.wait()
    pair.wait()

    def own_rows(r0, n):
        return pool[pl.ds((own0 + r0) // GROUP, n // GROUP)].reshape(n, width)

    def ring_copy(t):
        s = lax.rem(t, SLOTS)
        return pltpu.make_async_remote_copy(
            src_ref=cols.at[s, pl.ds(0, CHUNK)], dst_ref=recv.at[s], send_sem=ring_send.at[s], recv_sem=ring_recv.at[s],
            device_id={'row': nxt}, device_id_type=MESH)

    def sib_copy(t):
        s = lax.rem(t, SLOTS)
        return pltpu.make_async_remote_copy(
            src_ref=cols.at[s, pl.ds(0, CHUNK)], dst_ref=cols.at[s, pl.ds(CHUNK, CHUNK)],
            send_sem=sib_send.at[s], recv_sem=sib_recv.at[s], device_id={'row': sib}, device_id_type=MESH)

    last_send = steps - LAG

    def prep(t):
        s = lax.rem(t, SLOTS)
        for j in range(PER):
            cols[s, j * GROUP:(j + 1) * GROUP, :] = pool[tbl_ref[0, t * PER + j]]

    def take(t):
        ring_copy(t).wait_recv()
        dst = groups + lax.rem(t, fifo_chunks) * PER
        pool[pl.ds(dst, PER)] = recv[lax.rem(t, SLOTS)].reshape(PER, GROUP, width)

        @pl.when(t + SLOTS < last_send)
        def _():
            pl.semaphore_signal(ring_free, inc=1, device_id={'row': prv}, device_id_type=MESH)

    def col_vectors(t, masked):
        lane = lax.broadcasted_iota(jnp.int32, (1, 128), 1)
        low = lane < GROUP
        for half in range(2):
            for p in range(PER // 2):
                at = t * PER + 2 * p
                r0 = side_ref[tbl_ref[2 + half, at]].reshape(1, 128)
                r1 = side_ref[tbl_ref[2 + half, at + 1]].reshape(1, 128)
                dst = half * CHUNK + p * 128
                bc[0:1, dst:dst + 128] = jnp.where(low, r0, pltpu.roll(r1, GROUP, axis=1))
                bc[1:2, dst:dst + 128] = jnp.where(low, pltpu.roll(r0, GROUP, axis=1), r1)
                if masked:
                    i0 = tbl_ref[half, at] * GROUP - own0
                    i1 = tbl_ref[half, at + 1] * GROUP - own0 - GROUP
                    ids[0:1, dst:dst + 128] = jnp.where(low, i0, i1) + lane

    num_tiles = block // ROW_TILE

    def rows_of(m):
        return pl.ds(pl.multiple_of(m * ROW_TILE, ROW_TILE), ROW_TILE)

    def gram(m, s):
        return lax.dot_general(own_rows(m * ROW_TILE, ROW_TILE), cols[s], (((1,), (1,)), ((), ())),
                               preferred_element_type=jnp.float32)

    def weigh(g_ref, w_ref, m, masked):
        for part in range(0, ROW_TILE, SUB_TILE):
            rows = pl.ds(pl.multiple_of(m * ROW_TILE + part, SUB_TILE), SUB_TILE)
            sub = slice(part, part + SUB_TILE)
            a = a_ref[rows, :]
            c = c_ref[rows, :]
            if masked:
                rid = lax.broadcasted_iota(jnp.int32, (SUB_TILE, 128), 0) + (m * ROW_TILE + part)
            total = sacc[rows, :]
            for l in range(lane_groups):
                sl = slice(l * 128, (l + 1) * 128)
                e = jnp.minimum(g_ref[sub, sl] * gain + (a + bc[0:1, sl]), 0.0)
                w = (c * bc[1:2, sl]) * jnp.exp2(e)
                if masked:
                    w = jnp.where(rid == ids[0:1, sl], 0.0, w)
                total = total + w
                w_ref[sub, sl] = w.astype(jnp.bfloat16)
            sacc[rows, :] = total

    def pull(w_ref, m, s):
        rows = rows_of(m)
        out_ref[rows, :] += jnp.dot(w_ref[...], cols[s], preferred_element_type=jnp.float32)

    pairs = num_tiles // 2

    def body(t, i, masked):
        now = lax.rem(t, SLOTS)
        before = lax.rem(jnp.maximum(t - 1 + (i + pairs - 1) // pairs, 0), SLOTS)
        after = lax.rem(t + (i + 1) // pairs, SLOTS)
        g_b[...] = gram(2 * i + 1, now)
        weigh(g_a, w_a, 2 * i, masked)
        pull(w_b, lax.rem(2 * i - 1 + num_tiles, num_tiles), before)
        g_a[...] = gram(lax.rem(2 * i + 2, num_tiles), after)
        weigh(g_b, w_b, 2 * i + 1, masked)
        pull(w_a, 2 * i, now)

    def send(t):
        ring_live = t < last_send

        @pl.when(ring_live)
        def _():
            @pl.when(t >= SLOTS)
            def _():
                pl.semaphore_wait(ring_free, 1)
            ring_copy(t).start()

        @pl.when(t >= SLOTS)
        def _():
            pl.semaphore_wait(sib_free, 1)
        sib_copy(t).start()

    def done(t):
        @pl.when(t < last_send)
        def _():
            ring_copy(t).wait_send()
        sib_copy(t).wait_send()

        @pl.when(t + SLOTS < steps)
        def _():
            pl.semaphore_signal(sib_free, inc=1, device_id={'row': sib}, device_id_type=MESH)

    def step(t, masked):
        new = t + AHEAD

        @pl.when(new < steps)
        def _():
            @pl.when(new >= LAG)
            def _():
                take(new - LAG)
            prep(new)
        col_vectors(t, masked)

        @pl.when(new < steps)
        def _():
            send(new)

        def pair(i, carry):
            @pl.when((i == pairs - 1) & (t + 1 < steps))
            def _():
                sib_copy(t + 1).wait_recv()
            body(t, i, masked)
            return carry

        lax.fori_loop(0, pairs, pair, 0)

        @pl.when(t >= 1)
        def _():
            done(t - 1)

    own_steps = block // CHUNK
    for t in range(AHEAD):
        prep(t)
        send(t)
    sib_copy(0).wait_recv()
    g_a[...] = gram(0, 0)
    lax.fori_loop(0, own_steps, lambda t, c: (step(t, True), c)[1], 0)
    lax.fori_loop(own_steps, steps, lambda t, c: (step(t, False), c)[1], 0)
    pull(w_b, num_tiles - 1, (steps - 1) % SLOTS)
    done(steps - 1)

    def fold(m, acc):
        return acc + jnp.sum(sacc[pl.ds(pl.multiple_of(m * 128, 128), 128), :].reshape(16, 8, 128), axis=0)

    part = lax.fori_loop(0, block // 128, fold, jnp.zeros((8, 128), jnp.float32))
    part = jnp.sum(jnp.sum(part, axis=1, keepdims=True), axis=0, keepdims=True)
    esend[...] = jnp.broadcast_to(0.5 * part, esend.shape)
    inv = 1.0 / width

    def final(m, carry):
        r0 = pl.multiple_of(m * 128, 128)
        rows = pl.ds(r0, 128)
        x = own_rows(r0, 128).astype(jnp.float32)
        sums = jnp.sum(sacc[rows, :], axis=1, keepdims=True)
        out_ref[rows, :] = (sums * x - out_ref[rows, :]) * inv
        return carry

    copies = []
    for rel in range(1, num):
        copy = pltpu.make_async_remote_copy(
            src_ref=esend, dst_ref=ebuf.at[me], send_sem=e_send.at[rel], recv_sem=e_recv.at[me],
            device_id={'row': lax.rem(me + rel, num)}, device_id_type=MESH)
        copy.start()
        copies.append(copy)
    lax.fori_loop(0, block // 128, final, 0)
    ebuf[me] = esend[...]
    for rel in range(1, num):
        src = lax.rem(me + rel, num)
        pltpu.make_async_remote_copy(
            src_ref=esend, dst_ref=ebuf.at[src], send_sem=e_send.at[rel], recv_sem=e_recv.at[src],
            device_id={'row': src}, device_id_type=MESH).wait_recv()
    for copy in copies:
        copy.wait_send()
    en = ebuf[0]
    for j in range(1, num):
        en = en + ebuf[j]
    en_ref[0] = jnp.max(en)


def stream_tables(counts, me, num, block, total_steps):
    chips = num // 2
    zero_row = SIDE_ROWS - 1
    grp = (counts + (GROUP - 1)) // GROUP
    pairs = grp.reshape(chips, 2)
    first = pairs[:, 0]
    used = pairs[:, 0] + pairs[:, 1]
    half0 = (used + 1) // 2
    base = jnp.stack([jnp.zeros_like(half0), half0], axis=1)
    real = jnp.stack([half0, used - half0], axis=1)
    padded = jnp.maximum(real, LAG * PER)
    need = jnp.max(jnp.sum(padded, axis=0))
    need_steps = (need + PER - 1) // PER
    chip = me // 2
    core = me % 2
    pos = jnp.arange(total_steps * PER, dtype=jnp.int32)
    blk_groups = block // GROUP
    fifo_groups = 2 * blk_groups
    pools, sides = [], []
    for other in range(2):
        k = jnp.where(core == 1, 1 - other, other)
        hop = jnp.where(k == 0, chips - 1, 1)
        order = (chip + hop * jnp.arange(chips, dtype=jnp.int32)) % chips
        onehot = (order[:, None] == jnp.arange(chips)[None, :]).astype(jnp.int32)

        def pick(v):
            return jnp.sum(onehot * v[None, :], axis=1)
        seg_pad = pick(jnp.where(k == 0, padded[:, 0], padded[:, 1]))
        seg_real = pick(jnp.where(k == 0, real[:, 0], real[:, 1]))
        seg_base = pick(jnp.where(k == 0, base[:, 0], base[:, 1]))
        seg_first = pick(first)
        tri = (jnp.arange(chips)[None, :] < jnp.arange(chips)[:, None]).astype(jnp.int32)
        start = jnp.sum(tri * seg_pad[None, :], axis=1)
        inside = (pos[:, None] >= start[None, :]) & (pos[:, None] < (start + seg_pad)[None, :])
        off = pos[:, None] - start[None, :]
        live = inside & (off < seg_real[None, :])
        u = off + seg_base[None, :]
        in_a = u < seg_first[None, :]
        side = jnp.where(in_a, 2 * order[None, :] * SIDE_ROWS + u,
                         (2 * order[None, :] + 1) * SIDE_ROWS + u - seg_first[None, :])
        side = jnp.sum(jnp.where(live, side - zero_row, 0), axis=1) + zero_row
        own = jnp.where(in_a, u, blk_groups + u - seg_first[None, :])
        own = jnp.where(live[:, 0], own[:, 0], 0)
        pool = jnp.where(pos < seg_pad[0], own, fifo_groups + (pos - seg_pad[0]) % fifo_groups)
        pools.append(pool)
        sides.append(side)
    return jnp.stack(pools + sides).astype(jnp.int32), need_steps


def solution(mesh):
    num = mesh.shape['row']

    def per_device(positions, charges, counts):
        block, width = positions.shape
        me = lax.axis_index('row')
        pos_f32 = positions.astype(jnp.float32)
        scale = -0.5 * LOG2E / width
        a = jnp.sum(pos_f32 * pos_f32, axis=1) * scale
        live_q = jnp.where(jnp.arange(block) < counts[0], charges, 0.0)
        side = jnp.concatenate([a.reshape(-1, GROUP), live_q.reshape(-1, GROUP)], axis=1)
        extra = jnp.full((1, 128), counts[0].astype(jnp.float32))
        blk_groups = block // GROUP
        side = jnp.concatenate([side, extra, jnp.zeros((SIDE_ROWS - blk_groups - 1, 128), jnp.float32)], axis=0)
        vmem = pl.BlockSpec(memory_space=pltpu.VMEM)
        wide = jax.ShapeDtypeStruct((block, 128), jnp.float32)
        dma = pltpu.SemaphoreType.DMA
        x_own = positions.reshape(-1, GROUP, width)
        anywhere = pl.BlockSpec(memory_space=pl.ANY)
        everyone, a_wide, c_wide, x_sib = pl.pallas_call(
            functools.partial(exchange_kernel, num),
            out_shape=(jax.ShapeDtypeStruct((num, SIDE_ROWS, 128), jnp.float32), wide, wide,
                       jax.ShapeDtypeStruct(x_own.shape, x_own.dtype)),
            in_specs=[vmem, anywhere], out_specs=(vmem, vmem, vmem, anywhere),
            scratch_shapes=[dma((num // 2,)), dma((num,)), dma((num // 2,)), dma((num,)), dma, dma],
            compiler_params=pltpu.CompilerParams(collective_id=0, has_side_effects=True),
            name='exchange',
        )(side, x_own)
        all_counts = everyone[:, blk_groups, 0].astype(jnp.int32)
        own_steps = block // CHUNK
        max_steps = (num // 2) * own_steps
        tbl, need_steps = stream_tables(all_counts, me, num, block, max_steps)
        all_side = everyone.reshape(num * SIDE_ROWS, 128)

        def call(steps, cid):
            tile = functools.partial(pltpu.VMEM, (ROW_TILE, 2 * CHUNK))
            return pl.pallas_call(
                functools.partial(force_kernel, num, steps, block, width),
                out_shape=(jax.ShapeDtypeStruct((block, width), jnp.float32), jax.ShapeDtypeStruct((1,), jnp.float32)),
                in_specs=[pl.BlockSpec(memory_space=pltpu.SMEM), anywhere, anywhere, vmem, vmem, vmem],
                out_specs=(vmem, pl.BlockSpec(memory_space=pltpu.SMEM)),
                scratch_shapes=[
                    pltpu.VMEM((4 * block // GROUP, GROUP, width), jnp.bfloat16),
                    pltpu.VMEM((SLOTS, 2 * CHUNK, width), jnp.bfloat16),
                    pltpu.VMEM((SLOTS, CHUNK, width), jnp.bfloat16),
                    pltpu.VMEM((block, 128), jnp.float32),
                    pltpu.VMEM((8, 2 * CHUNK), jnp.float32),
                    pltpu.VMEM((8, 2 * CHUNK), jnp.int32),
                    pltpu.VMEM((8, 128), jnp.float32),
                    pltpu.VMEM((num, 8, 128), jnp.float32),
                    dma, dma, dma((SLOTS,)), dma((SLOTS,)), dma((SLOTS,)), dma((SLOTS,)),
                    dma((num,)), dma((num,)),
                    pltpu.SemaphoreType.REGULAR, pltpu.SemaphoreType.REGULAR,
                    tile(jnp.float32), tile(jnp.float32), tile(jnp.bfloat16), tile(jnp.bfloat16),
                ],
                compiler_params=pltpu.CompilerParams(
                    collective_id=cid, has_side_effects=True, vmem_limit_bytes=56 * 1024 * 1024),
                name='force',
            )(tbl, x_own, x_sib, all_side, a_wide, c_wide)

        choices = sorted({max(own_steps + 1, max_steps * part // 64) for part in STEP_PARTS})
        branch = sum((need_steps > steps).astype(jnp.int32) for steps in choices[:-1])
        forces, energy = lax.switch(branch, [functools.partial(call, steps, 1 + i) for i, steps in enumerate(choices)])
        return forces, energy

    row_spec = P(('sys', 'row'), None)
    vec_spec = P(('sys', 'row'))
    return jax.shard_map(per_device, mesh=mesh, in_specs=(row_spec, vec_spec, vec_spec), out_specs=(row_spec, P('sys')), check_vma=False)
```

```python
import functools
import math

import jax
import jax.numpy as jnp
from jax import lax
from jax.experimental import pallas as pl
from jax.experimental.pallas import tpu as pltpu
from jax.sharding import PartitionSpec as P

MESH = pl.DeviceIdType.MESH
GROUP = 64
CHUNK = 256
PER = CHUNK // GROUP
LAG = 2
AHEAD = 2
SLOTS = 8
ROW_TILE = 512
SUB_TILE = 64
SIDE_ROWS = 40
STEP_PARTS = (38, 40, 42, 44, 46, 49, 64)
LOG2E = math.log2(math.e)


def arrive(num, me):
    for rel in range(1, num):
        pl.semaphore_signal(pltpu.get_barrier_semaphore(), inc=1, device_id={'row': lax.rem(me + rel, num)},
                            device_id_type=MESH)


def exchange_kernel(num, side_ref, x_hbm, all_ref, a_wide, c_wide, x_sib,
                    send_sem, recv_sem, pass_send, pass_recv, x_send, x_recv):
    me = lax.axis_index('row')
    sib = me + 1 - 2 * lax.rem(me, 2)
    peers = [lax.rem(me + rel, num) for rel in range(2, num, 2)]
    barrier = pltpu.get_barrier_semaphore()
    for peer in peers + [sib]:
        pl.semaphore_signal(barrier, inc=1, device_id={'row': peer}, device_id_type=MESH)
    pl.semaphore_wait(barrier, len(peers) + 1)
    copies = []
    for n, peer in enumerate(peers):
        copy = pltpu.make_async_remote_copy(
            src_ref=side_ref, dst_ref=all_ref.at[me], send_sem=send_sem.at[n], recv_sem=recv_sem.at[me],
            device_id={'row': peer}, device_id_type=MESH)
        copy.start()
        copies.append(copy)
    own = pltpu.make_async_remote_copy(
        src_ref=side_ref, dst_ref=all_ref.at[me], send_sem=pass_send.at[len(peers)], recv_sem=pass_recv.at[me],
        device_id={'row': sib}, device_id_type=MESH)
    own.start()
    rows_out = pltpu.make_async_remote_copy(
        src_ref=x_hbm, dst_ref=x_sib, send_sem=x_send, recv_sem=x_recv, device_id={'row': sib}, device_id_type=MESH)
    rows_out.start()
    all_ref[me] = side_ref[...]
    low = lax.broadcasted_iota(jnp.int32, (1, 128), 1) < GROUP
    for r in range(a_wide.shape[0] // 128):
        rows = slice(r * 128, (r + 1) * 128)
        r0 = side_ref[2 * r:2 * r + 1, :]
        r1 = side_ref[2 * r + 1:2 * r + 2, :]
        a = jnp.where(low, r0, pltpu.roll(r1, GROUP, axis=1))
        c = jnp.where(low, pltpu.roll(r0, GROUP, axis=1), r1)
        a_wide[rows, :] = jnp.broadcast_to(a, (128, 128)).T
        c_wide[rows, :] = jnp.broadcast_to(c, (128, 128)).T
    for n, peer in enumerate(peers):
        pltpu.make_async_remote_copy(
            src_ref=side_ref, dst_ref=all_ref.at[peer], send_sem=send_sem.at[n], recv_sem=recv_sem.at[peer],
            device_id={'row': peer}, device_id_type=MESH).wait_recv()
        copy = pltpu.make_async_remote_copy(
            src_ref=all_ref.at[peer], dst_ref=all_ref.at[peer], send_sem=pass_send.at[n], recv_sem=pass_recv.at[peer],
            device_id={'row': sib}, device_id_type=MESH)
        copy.start()
        copies.append(copy)
    for src in [sib] + [lax.rem(sib + rel, num) for rel in range(2, num, 2)]:
        pltpu.make_async_remote_copy(
            src_ref=side_ref, dst_ref=all_ref.at[src], send_sem=pass_send.at[0], recv_sem=pass_recv.at[src],
            device_id={'row': sib}, device_id_type=MESH).wait_recv()
    own.wait_send()
    rows_out.wait()
    for copy in copies:
        copy.wait_send()


def force_kernel(num, steps, block, width, tbl_ref, x_hbm, x_sib, side_ref, a_ref, c_ref, out_ref, en_ref,
                 pool, cols, recv, sacc, bc, ids, esend, ebuf,
                 load_sem, pair_sem, ring_send, ring_recv, sib_send, sib_recv, e_send, e_recv,
                 ring_free, sib_free, g_a, g_b, w_a, w_b):
    me = lax.axis_index('row')
    core = lax.rem(me, 2)
    sib = me + 1 - 2 * core
    nxt = lax.rem(me + 2 * (1 - core) + (num - 2) * core, num)
    prv = lax.rem(me + (num - 2) * (1 - core) + 2 * core, num)
    fifo0 = 2 * block
    fifo_chunks = (2 * block) // CHUNK
    groups = fifo0 // GROUP
    own0 = core * block
    own_g = pl.ds(core * (block // GROUP), block // GROUP)
    sib_g = pl.ds((1 - core) * (block // GROUP), block // GROUP)
    gain = LOG2E / width
    lane_groups = 2 * CHUNK // 128

    arrive(num, me)
    load = pltpu.make_async_copy(x_hbm, pool.at[own_g], load_sem)
    load.start()
    pair = pltpu.make_async_copy(x_sib, pool.at[sib_g], pair_sem)
    pair.start()

    def clear(m, carry):
        rows = pl.ds(pl.multiple_of(m * 128, 128), 128)
        out_ref[rows, :] = jnp.zeros((128, width), jnp.float32)
        sacc[rows, :] = jnp.zeros((128, 128), jnp.float32)
        return carry

    lax.fori_loop(0, block // 128, clear, 0)
    w_b[...] = jnp.zeros_like(w_b)
    pl.semaphore_wait(pltpu.get_barrier_semaphore(), num - 1)
    load.wait()
    pair.wait()

    def own_rows(r0, n):
        return pool[pl.ds((own0 + r0) // GROUP, n // GROUP)].reshape(n, width)

    def ring_copy(t):
        s = lax.rem(t, SLOTS)
        return pltpu.make_async_remote_copy(
            src_ref=cols.at[s, pl.ds(0, CHUNK)], dst_ref=recv.at[s], send_sem=ring_send.at[s], recv_sem=ring_recv.at[s],
            device_id={'row': nxt}, device_id_type=MESH)

    def sib_copy(t):
        s = lax.rem(t, SLOTS)
        return pltpu.make_async_remote_copy(
            src_ref=cols.at[s, pl.ds(0, CHUNK)], dst_ref=cols.at[s, pl.ds(CHUNK, CHUNK)],
            send_sem=sib_send.at[s], recv_sem=sib_recv.at[s], device_id={'row': sib}, device_id_type=MESH)

    last_send = steps - LAG

    def prep(t):
        s = lax.rem(t, SLOTS)
        for j in range(PER):
            cols[s, j * GROUP:(j + 1) * GROUP, :] = pool[tbl_ref[0, t * PER + j]]

    def take(t):
        ring_copy(t).wait_recv()
        dst = groups + lax.rem(t, fifo_chunks) * PER
        pool[pl.ds(dst, PER)] = recv[lax.rem(t, SLOTS)].reshape(PER, GROUP, width)

        @pl.when(t + SLOTS < last_send)
        def _():
            pl.semaphore_signal(ring_free, inc=1, device_id={'row': prv}, device_id_type=MESH)

    def col_vectors(t, masked):
        lane = lax.broadcasted_iota(jnp.int32, (1, 128), 1)
        low = lane < GROUP
        for half in range(2):
            for p in range(PER // 2):
                at = t * PER + 2 * p
                r0 = side_ref[tbl_ref[2 + half, at]].reshape(1, 128)
                r1 = side_ref[tbl_ref[2 + half, at + 1]].reshape(1, 128)
                dst = half * CHUNK + p * 128
                bc[0:1, dst:dst + 128] = jnp.where(low, r0, pltpu.roll(r1, GROUP, axis=1))
                bc[1:2, dst:dst + 128] = jnp.where(low, pltpu.roll(r0, GROUP, axis=1), r1)
                if masked:
                    i0 = tbl_ref[half, at] * GROUP - own0
                    i1 = tbl_ref[half, at + 1] * GROUP - own0 - GROUP
                    ids[0:1, dst:dst + 128] = jnp.where(low, i0, i1) + lane

    num_tiles = block // ROW_TILE

    def rows_of(m):
        return pl.ds(pl.multiple_of(m * ROW_TILE, ROW_TILE), ROW_TILE)

    def gram(m, s):
        return lax.dot_general(own_rows(m * ROW_TILE, ROW_TILE), cols[s], (((1,), (1,)), ((), ())),
                               preferred_element_type=jnp.float32)

    def weigh(g_ref, w_ref, m, masked):
        for part in range(0, ROW_TILE, SUB_TILE):
            rows = pl.ds(pl.multiple_of(m * ROW_TILE + part, SUB_TILE), SUB_TILE)
            sub = slice(part, part + SUB_TILE)
            a = a_ref[rows, :]
            c = c_ref[rows, :]
            if masked:
                rid = lax.broadcasted_iota(jnp.int32, (SUB_TILE, 128), 0) + (m * ROW_TILE + part)
            total = sacc[rows, :]
            for l in range(lane_groups):
                sl = slice(l * 128, (l + 1) * 128)
                e = jnp.minimum(g_ref[sub, sl] * gain + (a + bc[0:1, sl]), 0.0)
                w = (c * bc[1:2, sl]) * jnp.exp2(e)
                if masked:
                    w = jnp.where(rid == ids[0:1, sl], 0.0, w)
                total = total + w
                w_ref[sub, sl] = w.astype(jnp.bfloat16)
            sacc[rows, :] = total

    def pull(w_ref, m, s):
        rows = rows_of(m)
        out_ref[rows, :] += jnp.dot(w_ref[...], cols[s], preferred_element_type=jnp.float32)

    pairs = num_tiles // 2

    def body(t, i, masked):
        now = lax.rem(t, SLOTS)
        before = lax.rem(jnp.maximum(t - 1 + (i + pairs - 1) // pairs, 0), SLOTS)
        after = lax.rem(t + (i + 1) // pairs, SLOTS)
        g_b[...] = gram(2 * i + 1, now)
        weigh(g_a, w_a, 2 * i, masked)
        pull(w_b, lax.rem(2 * i - 1 + num_tiles, num_tiles), before)
        g_a[...] = gram(lax.rem(2 * i + 2, num_tiles), after)
        weigh(g_b, w_b, 2 * i + 1, masked)
        pull(w_a, 2 * i, now)

    def send(t):
        ring_live = t < last_send

        @pl.when(ring_live)
        def _():
            @pl.when(t >= SLOTS)
            def _():
                pl.semaphore_wait(ring_free, 1)
            ring_copy(t).start()

        @pl.when(t >= SLOTS)
        def _():
            pl.semaphore_wait(sib_free, 1)
        sib_copy(t).start()

    def done(t):
        @pl.when(t < last_send)
        def _():
            ring_copy(t).wait_send()
        sib_copy(t).wait_send()

        @pl.when(t + SLOTS < steps)
        def _():
            pl.semaphore_signal(sib_free, inc=1, device_id={'row': sib}, device_id_type=MESH)

    def step(t, masked):
        new = t + AHEAD

        @pl.when(new < steps)
        def _():
            @pl.when(new >= LAG)
            def _():
                take(new - LAG)
            prep(new)
        col_vectors(t, masked)

        @pl.when(new < steps)
        def _():
            send(new)

        def pair(i, carry):
            @pl.when((i == pairs - 1) & (t + 1 < steps))
            def _():
                sib_copy(t + 1).wait_recv()
            body(t, i, masked)
            return carry

        lax.fori_loop(0, pairs, pair, 0)

        @pl.when(t >= 1)
        def _():
            done(t - 1)

    own_steps = block // CHUNK
    for t in range(AHEAD):
        prep(t)
        send(t)
    sib_copy(0).wait_recv()
    g_a[...] = gram(0, 0)
    lax.fori_loop(0, own_steps, lambda t, c: (step(t, True), c)[1], 0)
    lax.fori_loop(own_steps, steps, lambda t, c: (step(t, False), c)[1], 0)
    pull(w_b, num_tiles - 1, (steps - 1) % SLOTS)
    done(steps - 1)

    def fold(m, acc):
        return acc + jnp.sum(sacc[pl.ds(pl.multiple_of(m * 128, 128), 128), :].reshape(16, 8, 128), axis=0)

    part = lax.fori_loop(0, block // 128, fold, jnp.zeros((8, 128), jnp.float32))
    part = jnp.sum(jnp.sum(part, axis=1, keepdims=True), axis=0, keepdims=True)
    esend[...] = jnp.broadcast_to(0.5 * part, esend.shape)
    inv = 1.0 / width

    def final(m, carry):
        r0 = pl.multiple_of(m * 128, 128)
        rows = pl.ds(r0, 128)
        x = own_rows(r0, 128).astype(jnp.float32)
        sums = jnp.sum(sacc[rows, :], axis=1, keepdims=True)
        out_ref[rows, :] = (sums * x - out_ref[rows, :]) * inv
        return carry

    copies = []
    for rel in range(1, num):
        copy = pltpu.make_async_remote_copy(
            src_ref=esend, dst_ref=ebuf.at[me], send_sem=e_send.at[rel], recv_sem=e_recv.at[me],
            device_id={'row': lax.rem(me + rel, num)}, device_id_type=MESH)
        copy.start()
        copies.append(copy)
    lax.fori_loop(0, block // 128, final, 0)
    ebuf[me] = esend[...]
    for rel in range(1, num):
        src = lax.rem(me + rel, num)
        pltpu.make_async_remote_copy(
            src_ref=esend, dst_ref=ebuf.at[src], send_sem=e_send.at[rel], recv_sem=e_recv.at[src],
            device_id={'row': src}, device_id_type=MESH).wait_recv()
    for copy in copies:
        copy.wait_send()
    en = ebuf[0]
    for j in range(1, num):
        en = en + ebuf[j]
    en_ref[...] = en


def stream_tables(counts, me, num, block, total_steps):
    chips = num // 2
    zero_row = SIDE_ROWS - 1
    grp = (counts + (GROUP - 1)) // GROUP
    pairs = grp.reshape(chips, 2)
    first = pairs[:, 0]
    used = pairs[:, 0] + pairs[:, 1]
    half0 = (used + 1) // 2
    base = jnp.stack([jnp.zeros_like(half0), half0], axis=1)
    real = jnp.stack([half0, used - half0], axis=1)
    padded = jnp.maximum(real, LAG * PER)
    need = jnp.max(jnp.sum(padded, axis=0))
    need_steps = (need + PER - 1) // PER
    chip = me // 2
    core = me % 2
    pos = jnp.arange(total_steps * PER, dtype=jnp.int32)
    blk_groups = block // GROUP
    fifo_groups = 2 * blk_groups
    pools, sides = [], []
    for other in range(2):
        k = jnp.where(core == 1, 1 - other, other)
        hop = jnp.where(k == 0, chips - 1, 1)
        order = (chip + hop * jnp.arange(chips, dtype=jnp.int32)) % chips
        onehot = (order[:, None] == jnp.arange(chips)[None, :]).astype(jnp.int32)

        def pick(v):
            return jnp.sum(onehot * v[None, :], axis=1)
        seg_pad = pick(jnp.where(k == 0, padded[:, 0], padded[:, 1]))
        seg_real = pick(jnp.where(k == 0, real[:, 0], real[:, 1]))
        seg_base = pick(jnp.where(k == 0, base[:, 0], base[:, 1]))
        seg_first = pick(first)
        tri = (jnp.arange(chips)[None, :] < jnp.arange(chips)[:, None]).astype(jnp.int32)
        start = jnp.sum(tri * seg_pad[None, :], axis=1)
        inside = (pos[:, None] >= start[None, :]) & (pos[:, None] < (start + seg_pad)[None, :])
        off = pos[:, None] - start[None, :]
        live = inside & (off < seg_real[None, :])
        u = off + seg_base[None, :]
        in_a = u < seg_first[None, :]
        side = jnp.where(in_a, 2 * order[None, :] * SIDE_ROWS + u,
                         (2 * order[None, :] + 1) * SIDE_ROWS + u - seg_first[None, :])
        side = jnp.sum(jnp.where(live, side - zero_row, 0), axis=1) + zero_row
        own = jnp.where(in_a, u, blk_groups + u - seg_first[None, :])
        own = jnp.where(live[:, 0], own[:, 0], 0)
        pool = jnp.where(pos < seg_pad[0], own, fifo_groups + (pos - seg_pad[0]) % fifo_groups)
        pools.append(pool)
        sides.append(side)
    return jnp.stack(pools + sides).astype(jnp.int32), need_steps


def solution(mesh):
    num = mesh.shape['row']

    def per_device(positions, charges, counts):
        block, width = positions.shape
        me = lax.axis_index('row')
        pos_f32 = positions.astype(jnp.float32)
        scale = -0.5 * LOG2E / width
        a = jnp.sum(pos_f32 * pos_f32, axis=1) * scale
        live_q = jnp.where(jnp.arange(block) < counts[0], charges, 0.0)
        side = jnp.concatenate([a.reshape(-1, GROUP), live_q.reshape(-1, GROUP)], axis=1)
        extra = jnp.full((1, 128), counts[0].astype(jnp.float32))
        blk_groups = block // GROUP
        side = jnp.concatenate([side, extra, jnp.zeros((SIDE_ROWS - blk_groups - 1, 128), jnp.float32)], axis=0)
        vmem = pl.BlockSpec(memory_space=pltpu.VMEM)
        wide = jax.ShapeDtypeStruct((block, 128), jnp.float32)
        dma = pltpu.SemaphoreType.DMA
        x_own = positions.reshape(-1, GROUP, width)
        anywhere = pl.BlockSpec(memory_space=pl.ANY)
        everyone, a_wide, c_wide, x_sib = pl.pallas_call(
            functools.partial(exchange_kernel, num),
            out_shape=(jax.ShapeDtypeStruct((num, SIDE_ROWS, 128), jnp.float32), wide, wide,
                       jax.ShapeDtypeStruct(x_own.shape, x_own.dtype)),
            in_specs=[vmem, anywhere], out_specs=(vmem, vmem, vmem, anywhere),
            scratch_shapes=[dma((num // 2,)), dma((num,)), dma((num // 2,)), dma((num,)), dma, dma],
            compiler_params=pltpu.CompilerParams(collective_id=0, has_side_effects=True),
            name='exchange',
        )(side, x_own)
        all_counts = everyone[:, blk_groups, 0].astype(jnp.int32)
        own_steps = block // CHUNK
        max_steps = (num // 2) * own_steps
        tbl, need_steps = stream_tables(all_counts, me, num, block, max_steps)
        all_side = everyone.reshape(num * SIDE_ROWS, 128)

        def call(steps, cid):
            tile = functools.partial(pltpu.VMEM, (ROW_TILE, 2 * CHUNK))
            return pl.pallas_call(
                functools.partial(force_kernel, num, steps, block, width),
                out_shape=(jax.ShapeDtypeStruct((block, width), jnp.float32), jax.ShapeDtypeStruct((8, 128), jnp.float32)),
                in_specs=[pl.BlockSpec(memory_space=pltpu.SMEM), anywhere, anywhere, vmem, vmem, vmem],
                out_specs=(vmem, vmem),
                scratch_shapes=[
                    pltpu.VMEM((4 * block // GROUP, GROUP, width), jnp.bfloat16),
                    pltpu.VMEM((SLOTS, 2 * CHUNK, width), jnp.bfloat16),
                    pltpu.VMEM((SLOTS, CHUNK, width), jnp.bfloat16),
                    pltpu.VMEM((block, 128), jnp.float32),
                    pltpu.VMEM((8, 2 * CHUNK), jnp.float32),
                    pltpu.VMEM((8, 2 * CHUNK), jnp.int32),
                    pltpu.VMEM((8, 128), jnp.float32),
                    pltpu.VMEM((num, 8, 128), jnp.float32),
                    dma, dma, dma((SLOTS,)), dma((SLOTS,)), dma((SLOTS,)), dma((SLOTS,)),
                    dma((num,)), dma((num,)),
                    pltpu.SemaphoreType.REGULAR, pltpu.SemaphoreType.REGULAR,
                    tile(jnp.float32), tile(jnp.float32), tile(jnp.bfloat16), tile(jnp.bfloat16),
                ],
                compiler_params=pltpu.CompilerParams(
                    collective_id=cid, has_side_effects=True, vmem_limit_bytes=56 * 1024 * 1024),
                name='force',
            )(tbl, x_own, x_sib, all_side, a_wide, c_wide)

        choices = sorted({max(own_steps + 1, max_steps * part // 64) for part in STEP_PARTS})
        branch = sum((need_steps > steps).astype(jnp.int32) for steps in choices[:-1])
        forces, energy = lax.switch(branch, [functools.partial(call, steps, 1 + i) for i, steps in enumerate(choices)])
        return forces, energy[0, :1]

    row_spec = P(('sys', 'row'), None)
    vec_spec = P(('sys', 'row'))
    return jax.shard_map(per_device, mesh=mesh, in_specs=(row_spec, vec_spec, vec_spec), out_specs=(row_spec, P('sys')), check_vma=False)
```
